32 devices in a mesh: groups: 2 (over x), attn: 4 (over y, core), expert: 4 (over z).
Axes of the slice: x: 2, y: 2, z: 4, core: 2. Of those that a mesh axis runs over, the one named last changes fastest.
Arguments:
- tokens: bfloat16 [1024, 4096], P(('groups', 'attn'), 'expert'), parts along dimension 0, may hold values from -6 to 6
- expert_ids: int32 [1024, 8], P(('groups', 'attn')), parts along dimension 0, may hold values from 0 to 15, all different within a row; in each aligned block of 128 rows (0 to 127, 128 to 255, ...) at most 128 rows name the same one
- gate_weight: bfloat16 [1024, 8], P(('groups', 'attn')), parts along dimension 0, may hold values from 0.049804688 to 0.29882812
- w_gate: bfloat16 [16, 4096, 768], P('attn', 'expert'), may hold values from -0.09375 to 0.09375
- w_up: bfloat16 [16, 4096, 768], P('attn', 'expert'), may hold values from -0.09375 to 0.09375
- w_down: bfloat16 [16, 768, 4096], P('attn', None, 'expert'), may hold values from -0.21875 to 0.21875
- query: bfloat16 [64, 64, 128], P(('groups', 'attn', 'expert')), parts along dimension 0, may hold values from -100 to 100
- cache_k: bfloat16 [64, 768, 4, 128], P(('groups', 'attn', 'expert')), parts along dimension 0, may hold values from -6 to 6
- cache_v: bfloat16 [64, 768, 4, 128], P(('groups', 'attn', 'expert')), parts along dimension 0, may hold values from -6 to 6
- lengths: int32 [64], P(('groups', 'attn', 'expert')), parts along dimension 0, may hold values from 2 to 768, as said below
Outputs:
- moe_out: bfloat16 [1024, 4096], P(('groups', 'attn'), 'expert'), parts along dimension 0
- attn_out: bfloat16 [64, 8192], P(('groups', 'attn', 'expert')), parts along dimension 0
The draws below stay inside these ranges and needn't reach their ends.
There are 2 independent parts, one for each index of `groups`. The reference program is written for one: setup_inputs(seed, part) draws one part's arguments, and reference() takes and returns one part's arrays. A program takes and returns all parts, laid end to end along the dimension named above; an argument that names none is the same for every part. Nothing has to cross between parts.
Inputs may be any that keep to these rules, and one draw needn't show every extreme that they name: `expert_ids`: each row names 8 different experts. In the rows of one index of attn (aligned blocks of 128 rows) no expert is named by more than 128 rows, and in some block some expert by exactly 128. `lengths`: some sequence has all 768 positions live.
All inputs are finite; a program needn't handle non-finite values.
Results may differ from the reference program's by a relative error of at most 0.025.
Values may be sent and summed in bfloat16 or wider, within the bound.
A program may use at most 64 MiB of HBM per device.

```python
import math
import jax
import jax.numpy as jnp
import numpy as np
from jax import lax

D = 4096
FF = 768
TOPK = 8
TOK_DEV = 128
Q_HEADS = 64
KV_HEADS = 4
HEAD_DIM = 128
CTX = 768
EXPERTS = 16
TOKENS = 512
SEQS = 32
FEAT_DEV = 1024
CAPACITY = 256
SLOT = 128
N_EXPERT = 4


def attention_inputs(key):
    keys_key = jax.random.fold_in(key, 101)
    query_key = jax.random.fold_in(key, 102)
    shape_keys = (SEQS, CTX, KV_HEADS, HEAD_DIM)
    shape_query = (SEQS, Q_HEADS, HEAD_DIM)
    key_rows = jnp.clip(jax.random.normal(keys_key, shape_keys, jnp.float32), -6.0, 6.0)
    query_rows = jnp.clip(jax.random.normal(query_key, shape_query, jnp.float32), -6.0, 6.0)
    return (key_rows, query_rows)


def draw_query(key, part):
    return attention_inputs(key)[1].astype(jnp.bfloat16)


def draw_cache_k(key, part):
    return attention_inputs(key)[0].astype(jnp.bfloat16)


def draw_lengths(key, part):
    base_lengths = jax.random.randint(jax.random.fold_in(key, 201), (SEQS,), 2, CTX + 1, dtype=jnp.int32)
    full_index = jax.random.randint(jax.random.fold_in(key, 202), (), 0, SEQS, dtype=jnp.int32)
    return jnp.where(jnp.arange(SEQS, dtype=jnp.int32) == full_index, CTX, base_lengths).astype(jnp.int32)


def block_scale(own_key, shape, cuts, smallest, top_value):
    factor_of = 1.0
    for axis_at, shards_of in cuts:
        steps = jax.random.uniform(jax.random.fold_in(jax.random.fold_in(own_key, 6), axis_at), (shards_of,), jnp.float32, smallest / len(cuts), top_value / len(cuts))
        factor_of = factor_of * jnp.repeat(jnp.exp(steps), shape[axis_at] // shards_of).reshape((-1,) + (1,) * (len(shape) - 1 - axis_at))
    return factor_of


def deal_out(stream_key, own, number, rows, count, top, most, slope):
    order = jax.random.permutation(stream_key, count)
    crowded, ordinary = shares(count, rows * top, most, slope, True), shares(count, rows * top, most, slope, False)
    places = jnp.arange(count)

    def named(sizes, offset_by):
        used = int((sizes > 0).sum())
        fixed = max(1, used // 4)
        passed = fixed + (places - fixed + offset_by * (used - fixed)) % max(1, count - fixed)
        return jnp.zeros((count,), jnp.int32).at[order[jnp.where(places < fixed, places, passed)]].set(jnp.asarray(sizes, jnp.int32))

    sizes = jnp.where(number % 4 == 0, named(crowded, number // 4), named(ordinary, number - number // 4 - 1))
    mixed = jax.random.permutation(jax.random.fold_in(own, 3), count)
    donor, taker = mixed[0:count // 2 * 2:2], mixed[1:count // 2 * 2:2]
    margin = jnp.minimum(sizes[donor] - 1, most - sizes[taker]) // 2
    margin = jnp.where((donor == order[0]) | (taker == order[0]) | (sizes[taker] == 0), 0, jnp.maximum(margin, 0))
    passed = jax.random.randint(jax.random.fold_in(own, 4), (count // 2,), 0, 1 << 20) % (margin + 1)
    sizes = sizes.at[donor].add(-passed).at[taker].add(passed)
    items = jnp.searchsorted(jnp.cumsum(sizes), jnp.arange(rows * top), side="right").astype(jnp.int32)
    table = items.reshape(top, rows).T
    table = table[jax.random.permutation(jax.random.fold_in(own, 1), rows)]
    offset_by = jax.random.randint(jax.random.fold_in(own, 2), (rows, 1), 0, top)
    return jnp.take_along_axis(table, (jnp.arange(top)[None, :] + offset_by) % top, axis=1)


def shares(number_of, total, reach, slope, full):
    portions = [(1 << 20) // math.isqrt(rank ** slope) + 1 for rank in range(1, number_of + 1)]
    largest = reach if full else min(reach, max(-(-total // number_of), total * portions[0] // sum(portions)))
    least = 1 if total - largest >= number_of - 1 else 0
    given, rest = [largest] + [least] * (number_of - 1), total - largest - least * (number_of - 1)
    while rest > 0:
        movable = [i for i in range(1, number_of) if given[i] < largest] or [i for i in range(1, number_of) if given[i] < reach]
        mass, remaining = sum([portions[i] for i in movable]), rest
        for i in movable:
            addition = min(reach - given[i], max(1, remaining * portions[i] // mass), rest)
            given[i] = given[i] + addition
            rest = rest - addition
    return np.array(given)


def centred(rng, extent, scale, reach, split=(), held_as=jnp.bfloat16):
    values = scale * jax.random.normal(rng, extent, jnp.float32)
    if split:
        values = values * block_scale(rng, extent, split, -0.22, 0.18)
    return jnp.clip(values, -reach, reach).astype(held_as)


def setup_inputs(seed: int = 0, part: int = 0) -> dict:
    keys = jax.random.split(jax.random.key(seed), 11)
    own_keys = jax.random.split(jax.random.fold_in(keys[10], part), 11)
    tokens = centred(own_keys[0], (TOKENS, D), 1.0, 6.0, ((0, 4), (1, 4)))
    expert_ids_keys = jax.random.split(jax.random.fold_in(own_keys[1], 1), TOKENS // TOK_DEV)
    expert_ids_turns = jax.random.permutation(jax.random.fold_in(own_keys[1], 3), TOKENS // TOK_DEV)
    expert_ids = jax.vmap(lambda own, number: deal_out(jax.random.fold_in(own_keys[1], 2), own, number, TOK_DEV, EXPERTS, TOPK, SLOT, 2))(expert_ids_keys, expert_ids_turns).reshape((TOKENS, TOPK))
    gate_weight = jnp.clip(0.049804688 + 0.24902344 * jax.random.uniform(own_keys[2], (TOKENS, TOPK), jnp.float32) ** block_scale(own_keys[2], (TOKENS, TOPK), ((0, 4),), -0.2, 0.2), 0.049804688, 0.29882812).astype(jnp.bfloat16)
    w_gate = centred(keys[3], (EXPERTS, D, FF), D ** -0.5, 0.09375, ((0, 4), (1, 4)))
    w_up = centred(keys[4], (EXPERTS, D, FF), D ** -0.5, 0.09375, ((0, 4), (1, 4)))
    w_down = centred(keys[5], (EXPERTS, FF, D), FF ** -0.5, 0.21875, ((0, 4), (2, 4)))
    query = draw_query(jax.random.fold_in(jax.random.fold_in(keys[10], part), 71), part)
    cache_k = draw_cache_k(jax.random.fold_in(jax.random.fold_in(keys[10], part), 71), part)
    cache_v = centred(own_keys[8], (SEQS, CTX, KV_HEADS, HEAD_DIM), 1.0, 6.0, ((0, 16),))
    lengths = draw_lengths(jax.random.fold_in(jax.random.fold_in(keys[10], part), 71), part)
    return {"tokens": tokens, "expert_ids": expert_ids, "gate_weight": gate_weight, "w_gate": w_gate, "w_up": w_up, "w_down": w_down, "query": query, "cache_k": cache_k, "cache_v": cache_v, "lengths": lengths}


def one_expert(operands):
    expert_rows, gate_mat, up_mat, down_mat = operands
    blocked = expert_rows.astype(jnp.float32).reshape(CAPACITY, N_EXPERT, FEAT_DEV)
    both_mats = jnp.concatenate([gate_mat, up_mat], axis=1).astype(jnp.float32).reshape(N_EXPERT, FEAT_DEV, 2 * FF)
    partials = jnp.einsum("rbd,bdf->brf", blocked, both_mats)
    rounded = lax.optimization_barrier(partials.astype(jnp.bfloat16))
    both_sums = jnp.sum(rounded.astype(jnp.float32), axis=0)
    hidden = (jax.nn.silu(both_sums[:, :FF]) * both_sums[:, FF:]).astype(jnp.bfloat16)
    return jnp.dot(hidden, down_mat, preferred_element_type=jnp.float32).astype(jnp.bfloat16)


def reference(tokens, expert_ids, gate_weight, w_gate, w_up, w_down, query, cache_k, cache_v, lengths):
    total_rows = tokens.shape[0]
    experts = w_gate.shape[0]
    wanted = jnp.arange(experts, dtype=jnp.int32)
    member = jnp.any(expert_ids[:, :, None] == wanted[None, None, :], axis=1).astype(jnp.int32)
    position = jnp.cumsum(member, axis=0, dtype=jnp.int32) - member
    taken = (member > 0) & (position < CAPACITY)
    target = jnp.where(taken, wanted[None, :] * CAPACITY + position, experts * CAPACITY)
    owners = jnp.broadcast_to(jnp.arange(total_rows, dtype=jnp.int32)[:, None], (total_rows, experts))
    token_index = jnp.full((experts * CAPACITY,), total_rows, jnp.int32).at[target.reshape(-1)].set(owners.reshape(-1), mode="drop")
    padded = jnp.concatenate([tokens, jnp.zeros((1, D), tokens.dtype)], axis=0)
    packed = padded[token_index].reshape(experts, CAPACITY, D)
    results = lax.map(one_expert, (packed, w_gate, w_up, w_down))
    results = lax.optimization_barrier(results)
    place_of = jnp.take_along_axis(position, expert_ids, axis=1)
    keep_mask = place_of < CAPACITY
    flat_index = jnp.where(keep_mask, expert_ids * CAPACITY + place_of, 0)
    picked = results.reshape(experts * CAPACITY, D)[flat_index]
    factor = jnp.where(keep_mask, gate_weight.astype(jnp.float32), 0.0)
    moe_out = jnp.sum(factor[:, :, None] * picked.astype(jnp.float32), axis=1).astype(jnp.bfloat16)

    seq_count = query.shape[0]
    grouped = query.astype(jnp.float32).reshape(seq_count, KV_HEADS, Q_HEADS // KV_HEADS, HEAD_DIM)
    scores = jnp.einsum("skgd,slkd->skgl", grouped, cache_k.astype(jnp.float32)) * (HEAD_DIM ** -0.5)
    live_mask = jnp.arange(CTX, dtype=jnp.int32)[None, None, None, :] < lengths[:, None, None, None]
    masked = jnp.where(live_mask, scores, -jnp.inf)
    row_peak = jnp.max(masked, axis=3, keepdims=True)
    weighted = jnp.exp(masked - row_peak)
    denominator = jnp.sum(weighted, axis=3, keepdims=True)
    prob_bf = lax.optimization_barrier((weighted / denominator).astype(jnp.bfloat16))
    attended = jnp.einsum("skgl,slkd->skgd", prob_bf.astype(jnp.float32), cache_v.astype(jnp.float32))
    attn_out = attended.reshape(seq_count, Q_HEADS * HEAD_DIM).astype(jnp.bfloat16)
    return (moe_out, attn_out)
```

```python
import functools

import jax
import jax.numpy as jnp
from jax import lax
from jax.experimental import pallas as pl
from jax.experimental.pallas import tpu as pltpu
from jax.sharding import PartitionSpec as P

F32 = jnp.float32
BF16 = jnp.bfloat16
I32 = jnp.int32

TOKEN_CUTS = 4
CHUNK_ROWS = 16
LAG = 3
RETURN_CUTS = 4


def remote(src, dst, send_sem, recv_sem, axis, peer):
    return pltpu.make_async_remote_copy(
        src_ref=src,
        dst_ref=dst,
        send_sem=send_sem,
        recv_sem=recv_sem,
        device_id={axis: peer},
        device_id_type=pl.DeviceIdType.MESH,
    )


def attend(s, length, query_ref, ck_ref, cv_ref, att_ref, kv_count):
    _, heads, size = query_ref.shape
    span = ck_ref.shape[1]
    column = lax.broadcasted_iota(I32, (heads, span), 1)
    row = lax.broadcasted_iota(I32, (heads, span), 0)
    own = lax.rem(column, kv_count) == row // (heads // kv_count)
    scores = lax.dot_general(
        query_ref[s], ck_ref[s], (((1,), (1,)), ((), ())),
        preferred_element_type=F32,
    ) * size ** (-0.5)
    live = own & (column < length * kv_count)
    masked = jnp.where(live, scores, -jnp.inf)
    peak = jnp.max(masked, axis=1, keepdims=True)
    weighted = jnp.exp(masked - peak)
    prob = (weighted / jnp.sum(weighted, axis=1, keepdims=True)).astype(BF16)
    att_ref[s] = jnp.dot(prob, cv_ref[s], preferred_element_type=F32).astype(BF16)


def moe_kernel(
    n_attn,
    n_exp,
    experts,
    kv_count,
    tok_hbm,
    ids_hbm,
    gw_hbm,
    wg_hbm,
    wu_hbm,
    wd_hbm,
    length_hbm,
    query_hbm,
    ck_hbm,
    cv_hbm,
    out_ref,
    att_ref,
    wg,
    wu,
    wd,
    ck,
    cv,
    query,
    length,
    tok_all,
    ids_all,
    gw_all,
    pos,
    gate_of,
    part,
    part_in,
    hid,
    acc,
    ret1,
    ret1_in,
    ret2,
    ret2_in,
    w_sem,
    c_sem,
    ids_s,
    ids_r,
    gw_s,
    gw_r,
    far_s,
    far_r,
    near_s,
    near_r,
    part_s,
    part_r,
    hid_s,
    hid_r,
    ret1_s,
    ret1_r,
    ret2_s,
    ret2_r,
):
    me = lax.axis_index("attn")
    mine = lax.axis_index("expert")
    lane = lax.rem(me, 2)
    line = me // 2
    lines = n_attn // 2
    partner = me + 1 - 2 * lane
    last = n_exp - 1
    local = wg.shape[0]
    rows, feat = tok_all.shape[1:]
    ffn = wg.shape[2]
    feat_out = wd.shape[2]
    topk = ids_all.shape[1]
    half = part.shape[2]
    capacity = 2 * half
    all_rows = n_attn * rows
    per = half // CHUNK_ROWS
    chunks = local * per
    cut = feat // TOKEN_CUTS
    out_cut = feat_out // RETURN_CUTS

    def at_line(other):
        return lax.rem(other + 2 * lines, lines)

    tok_copy = pltpu.make_async_copy(tok_hbm, tok_all.at[me], c_sem.at[0])
    ids_copy = pltpu.make_async_copy(ids_hbm, ids_all.at[me], c_sem.at[1])
    gw_copy = pltpu.make_async_copy(gw_hbm, gw_all.at[me], c_sem.at[2])
    len_copy = pltpu.make_async_copy(length_hbm, length, c_sem.at[3])
    query_copy = pltpu.make_async_copy(query_hbm, query, c_sem.at[4])
    ck_copy = pltpu.make_async_copy(ck_hbm, ck, c_sem.at[5])
    cv_copy = pltpu.make_async_copy(cv_hbm, cv, c_sem.at[6])
    for copy in (ids_copy, gw_copy, tok_copy, len_copy, query_copy, ck_copy, cv_copy):
        copy.start()

    def weight_copy(i, j):
        src, dst = ((wg_hbm, wg), (wu_hbm, wu), (wd_hbm, wd))[i]
        return pltpu.make_async_copy(src.at[j], dst.at[j], w_sem.at[i, j])

    for j in range(local):
        weight_copy(0, j).start()
        weight_copy(1, j).start()
    for j in range(local):
        weight_copy(2, j).start()

    barrier = pltpu.get_barrier_semaphore()
    for d in range(1, n_attn):
        pl.semaphore_signal(
            barrier, inc=1, device_id={"attn": lax.rem(me + d, n_attn)},
            device_id_type=pl.DeviceIdType.MESH,
        )

    @pl.when(mine > 0)
    def _():
        pl.semaphore_signal(
            barrier, inc=1, device_id={"expert": mine - 1},
            device_id_type=pl.DeviceIdType.MESH,
        )

    @pl.when(mine < last)
    def _():
        pl.semaphore_signal(
            barrier, inc=1, device_id={"expert": mine + 1},
            device_id_type=pl.DeviceIdType.MESH,
        )

    ends = jnp.where(mine > 0, 1, 0) + jnp.where(mine < last, 1, 0)
    ids_copy.wait()
    gw_copy.wait()
    tok_copy.wait()
    pl.semaphore_wait(barrier, n_attn - 1 + ends)

    def ids_send(d, slot):
        return remote(ids_all.at[slot], ids_all.at[slot], ids_s.at[d - 1], ids_r.at[d - 1],
                      "attn", lax.rem(me + d, n_attn))

    def gw_send(d, slot):
        return remote(gw_all.at[slot], gw_all.at[slot], gw_s.at[d - 1], gw_r.at[d - 1],
                      "attn", lax.rem(me + d, n_attn))

    def far(d, q, block):
        view = tok_all.at[block, :, pl.ds(q * cut, cut)]
        return remote(view, view, far_s.at[d - 1, q], far_r.at[d - 1, q],
                      "attn", at_line(line + d) * 2 + lane)

    def near(d, q, block):
        view = tok_all.at[block, :, pl.ds(q * cut, cut)]
        return remote(view, view, near_s.at[d, q], near_r.at[d, q], "attn", partner)

    def sender(d):
        return at_line(line - d) * 2 + lane

    for d in range(1, n_attn):
        ids_send(d, me).start()
        gw_send(d, me).start()
    for q in range(TOKEN_CUTS):
        for d in range(1, lines):
            far(d, q, me).start()
    for q in range(TOKEN_CUTS):
        near(0, q, me).start()

    acc[...] = jnp.zeros_like(acc)

    for d in range(1, n_attn):
        ids_send(d, lax.rem(me + n_attn - d, n_attn)).wait_recv()
        gw_send(d, lax.rem(me + n_attn - d, n_attn)).wait_recv()

    before = (
        lax.broadcasted_iota(I32, (rows, rows), 0)
        < lax.broadcasted_iota(I32, (rows, rows), 1)
    ).astype(F32).astype(BF16)
    names = lax.broadcasted_iota(I32, (experts, rows), 0)
    offset = jnp.zeros((experts, 1), F32)
    for b in range(n_attn):
        member = jnp.zeros((experts, rows), F32)
        factor = jnp.zeros((experts, rows), F32)
        wide = gw_all[b].astype(F32)
        for k in range(topk):
            hit = names == ids_all[b, k:k + 1, :]
            member = jnp.where(hit, 1.0, member)
            factor = jnp.where(hit, wide[k:k + 1, :], factor)
        place = jnp.dot(member.astype(BF16), before, preferred_element_type=F32) + offset
        offset = offset + jnp.sum(member, axis=1, keepdims=True)
        pos[:, b * rows:(b + 1) * rows] = jnp.where(member > 0.5, place, -1.0).astype(I32)
        gate_of[:, b * rows:(b + 1) * rows] = factor

    len_copy.wait()
    query_copy.wait()
    ck_copy.wait()
    cv_copy.wait()
    relay = [(d, q) for q in range(TOKEN_CUTS) for d in range(1, lines)]
    seqs = query.shape[0]
    done = 0
    for s in range(seqs):
        attend(s, length[s], query, ck, cv, att_ref, kv_count)
        until = len(relay) * (s + 1) // (seqs + 1)
        for d, q in relay[done:until]:
            far(d, q, sender(d)).wait_recv()
            near(d, q, sender(d)).start()
        done = until
    for d, q in relay[done:]:
        far(d, q, sender(d)).wait_recv()
        near(d, q, sender(d)).start()
    for q in range(TOKEN_CUTS):
        for d in range(lines):
            near(d, q, at_line(line - d) * 2 + 1 - lane).wait_recv()

    def steps_from(way):
        return mine if way == 0 else last - mine

    def piece(ref, way, k):
        j = k // per
        first_row = pl.multiple_of(lax.rem(k, per) * CHUNK_ROWS, CHUNK_ROWS)
        return ref.at[j, way, pl.ds(first_row, CHUNK_ROWS)]

    def part_copy(way, k):
        return remote(piece(part, way, k), piece(part_in, way, k),
                      part_s.at[way, k // per], part_r.at[way, k],
                      "expert", lax.rem(mine + 1 - 2 * way + n_exp, n_exp))

    def hid_copy(way, k):
        return remote(piece(hid, way, k), piece(hid, way, k),
                      hid_s.at[way, k // per], hid_r.at[way, k],
                      "expert", lax.rem(mine - 1 + 2 * way + n_exp, n_exp))

    def first(j, carry):
        place = pos[pl.ds(me * local + j, 1), :]
        chosen = lax.broadcasted_iota(I32, (capacity, all_rows), 0) == place
        packed = jnp.dot(
            chosen.astype(F32).astype(BF16),
            tok_all[...].reshape(all_rows, feat),
            preferred_element_type=F32,
        ).astype(BF16)
        weight_copy(0, j).wait()
        weight_copy(1, j).wait()
        gate = jnp.dot(packed, wg[j], preferred_element_type=F32).astype(BF16)
        part[j, :, :, :ffn] = gate.reshape(2, half, ffn)
        up = jnp.dot(packed, wu[j], preferred_element_type=F32).astype(BF16)
        part[j, :, :, ffn:] = up.reshape(2, half, ffn)
        for way in range(2):
            @pl.when(steps_from(way) == 0)
            def _():
                for r in range(per):
                    part_copy(way, j * per + r).start()
        return carry

    lax.fori_loop(0, local, first, 0)

    def reduce(way, k):
        part_copy(way, k).wait_recv()
        total = piece(part, way, k)[...].astype(F32) + piece(part_in, way, k)[...].astype(F32)

        @pl.when(steps_from(way) < last)
        def _():
            piece(part, way, k)[...] = total.astype(BF16)
            part_copy(way, k).start()

        @pl.when(steps_from(way) == last)
        def _():
            gate = total[:, :ffn]
            piece(hid, way, k)[...] = (
                gate / (1.0 + jnp.exp(-gate)) * total[:, ffn:]
            ).astype(BF16)
            hid_copy(way, k).start()

    def reduce_step(s, carry):
        for way in range(2):
            k = s - LAG * (steps_from(way) - 1)

            @pl.when((steps_from(way) > 0) & (k >= 0) & (k < chunks))
            def _():
                reduce(way, k)
        return carry

    lax.fori_loop(0, chunks + LAG * (last - 1), reduce_step, 0)

    def pass_on(k, carry):
        for way in range(2):
            @pl.when(steps_from(way) < last)
            def _():
                hid_copy(way, k).wait_recv()

            @pl.when((steps_from(way) < last) & (steps_from(way) > 0))
            def _():
                hid_copy(way, k).start()
        return carry

    def second(j, carry):
        lax.fori_loop(j * per, (j + 1) * per, pass_on, 0)
        weight_copy(2, j).wait()
        result = jnp.dot(
            hid[j].reshape(capacity, ffn), wd[j], preferred_element_type=F32
        ).astype(BF16)
        place = pos[pl.ds(me * local + j, 1), :]
        factor = gate_of[pl.ds(me * local + j, 1), :]
        slots = lax.broadcasted_iota(I32, (capacity, all_rows), 0)
        spread = jnp.where(slots == place, factor, 0.0).astype(BF16)
        acc[...] += lax.dot_general(
            spread, result, (((0,), (0,)), ((), ())), preferred_element_type=F32
        )
        return carry

    lax.fori_loop(0, local, second, 0)

    def block(index, q):
        return acc[pl.ds(pl.multiple_of(index * rows, rows), rows), q * out_cut:(q + 1) * out_cut]

    def ret1_copy(q):
        columns = pl.ds(q * out_cut, out_cut)
        return remote(ret1.at[:, :, columns], ret1_in.at[:, :, columns],
                      ret1_s.at[q], ret1_r.at[q], "attn", partner)

    def ret2_copy(d, q):
        columns = pl.ds(q * out_cut, out_cut)
        return remote(ret2.at[d - 1, :, columns], ret2_in.at[d - 1, :, columns],
                      ret2_s.at[d - 1, q], ret2_r.at[d - 1, q],
                      "attn", at_line(line + d) * 2 + lane)

    for q in range(RETURN_CUTS):
        columns = slice(q * out_cut, (q + 1) * out_cut)
        for y in range(lines):
            ret1[y, :, columns] = block(2 * y + 1 - lane, q).astype(BF16)
        ret1_copy(q).start()
    for q in range(RETURN_CUTS):
        columns = slice(q * out_cut, (q + 1) * out_cut)
        ret1_copy(q).wait_recv()
        for d in range(1, lines):
            to = at_line(line + d)
            ret2[d - 1, :, columns] = (
                block(2 * to + lane, q) + ret1_in[to, :, columns].astype(F32)
            ).astype(BF16)
            ret2_copy(d, q).start()
    for q in range(RETURN_CUTS):
        columns = slice(q * out_cut, (q + 1) * out_cut)
        total = block(me, q) + ret1_in[line, :, columns].astype(F32)
        for d in range(1, lines):
            ret2_copy(d, q).wait_recv()
            total = total + ret2_in[d - 1, :, columns].astype(F32)
        out_ref[:, columns] = total.astype(BF16)

    for d in range(1, n_attn):
        ids_send(d, me).wait_send()
        gw_send(d, me).wait_send()
    for q in range(TOKEN_CUTS):
        near(0, q, me).wait_send()
        for d in range(1, lines):
            far(d, q, me).wait_send()
            near(d, q, sender(d)).wait_send()
    for q in range(RETURN_CUTS):
        ret1_copy(q).wait_send()
        for d in range(1, lines):
            ret2_copy(d, q).wait_send()

    for way in range(2):
        for j in range(local):
            @pl.when(steps_from(way) < last)
            def _():
                remote(part.at[j, way], part_in.at[j, way], part_s.at[way, j], part_r.at[way, 0],
                       "expert", lax.rem(mine + 1 - 2 * way + n_exp, n_exp)).wait_send()

            @pl.when(steps_from(way) > 0)
            def _():
                remote(hid.at[j, way], hid.at[j, way], hid_s.at[way, j], hid_r.at[way, 0],
                       "expert", lax.rem(mine - 1 + 2 * way + n_exp, n_exp)).wait_send()


def routed(tokens, expert_ids, gate_weight, w_gate, w_up, w_down, query, cache_k, cache_v, lengths, n_attn, n_exp):
    rows, feat = tokens.shape
    local, _, ffn = w_gate.shape
    feat_out = w_down.shape[2]
    topk = expert_ids.shape[1]
    experts = local * n_attn
    capacity = rows * topk // local
    half = capacity // 2
    lines = n_attn // 2
    chunks = local * (half // CHUNK_ROWS)
    seqs, heads, size = query.shape
    context, kv_count = cache_k.shape[1:3]
    flat = (seqs, context * kv_count, size)
    dma = pltpu.SemaphoreType.DMA
    vmem = pltpu.VMEM
    return pl.pallas_call(
        functools.partial(moe_kernel, n_attn, n_exp, experts, kv_count),
        out_shape=(
            jax.ShapeDtypeStruct((rows, feat_out), BF16),
            jax.ShapeDtypeStruct(query.shape, BF16),
        ),
        in_specs=[pl.BlockSpec(memory_space=pltpu.HBM)] * 10,
        out_specs=[pl.BlockSpec(memory_space=pltpu.VMEM)] * 2,
        scratch_shapes=[
            vmem(w_gate.shape, BF16),
            vmem(w_up.shape, BF16),
            vmem(w_down.shape, BF16),
            vmem(flat, BF16),
            vmem(flat, BF16),
            vmem(query.shape, BF16),
            pltpu.SMEM(lengths.shape, I32),
            vmem((n_attn, rows, feat), BF16),
            vmem((n_attn, topk, rows), I32),
            vmem((n_attn, topk, rows), BF16),
            vmem((experts, n_attn * rows), I32),
            vmem((experts, n_attn * rows), F32),
            vmem((local, 2, half, 2 * ffn), BF16),
            vmem((local, 2, half, 2 * ffn), BF16),
            vmem((local, 2, half, ffn), BF16),
            vmem((n_attn * rows, feat_out), F32),
            vmem((lines, rows, feat_out), BF16),
            vmem((lines, rows, feat_out), BF16),
            vmem((lines - 1, rows, feat_out), BF16),
            vmem((lines - 1, rows, feat_out), BF16),
            dma((3, local)),
            dma((7,)),
            dma((n_attn - 1,)),
            dma((n_attn - 1,)),
            dma((n_attn - 1,)),
            dma((n_attn - 1,)),
            dma((lines - 1, TOKEN_CUTS)),
            dma((lines - 1, TOKEN_CUTS)),
            dma((lines, TOKEN_CUTS)),
            dma((lines, TOKEN_CUTS)),
            dma((2, local)),
            dma((2, chunks)),
            dma((2, local)),
            dma((2, chunks)),
            dma((RETURN_CUTS,)),
            dma((RETURN_CUTS,)),
            dma((lines - 1, RETURN_CUTS)),
            dma((lines - 1, RETURN_CUTS)),
        ],
        compiler_params=pltpu.CompilerParams(
            collective_id=0, has_side_effects=True, vmem_limit_bytes=56 * 1024 * 1024
        ),
    )(
        tokens, expert_ids.T, gate_weight.T, w_gate, w_up, w_down, lengths, query,
        cache_k.reshape(flat), cache_v.reshape(flat),
    )


def body(tokens, expert_ids, gate_weight, w_gate, w_up, w_down, query, cache_k, cache_v, lengths):
    n_attn = lax.axis_size("attn")
    n_exp = lax.axis_size("expert")
    moe_out, attended = routed(
        tokens, expert_ids, gate_weight, w_gate, w_up, w_down,
        query, cache_k, cache_v, lengths, n_attn, n_exp,
    )
    attn_out = attended.reshape(query.shape[0], -1)
    return (moe_out, attn_out)


def solution(mesh):
    return jax.shard_map(
        body,
        mesh=mesh,
        in_specs=(
            P(("groups", "attn"), "expert"),
            P(("groups", "attn"), None),
            P(("groups", "attn"), None),
            P("attn", "expert", None),
            P("attn", "expert", None),
            P("attn", None, "expert"),
            P(("groups", "attn", "expert"), None, None),
            P(("groups", "attn", "expert"), None, None, None),
            P(("groups", "attn", "expert"), None, None, None),
            P(("groups", "attn", "expert")),
        ),
        out_specs=(P(("groups", "attn"), "expert"), P(("groups", "attn", "expert"), None)),
        check_vma=False,
    )
```

```python
import functools

import jax
import jax.numpy as jnp
from jax import lax
from jax.experimental import pallas as pl
from jax.experimental.pallas import tpu as pltpu
from jax.sharding import PartitionSpec as P

F32 = jnp.float32
BF16 = jnp.bfloat16
I32 = jnp.int32

TOKEN_CUTS = 4
CHUNK_ROWS = 16
LAG = 3
HLAG = 8
PACE = 2
FIRST_STEPS = 1
RETURN_CUTS = 4
RETURN_DELAY = 2


def remote(src, dst, send_sem, recv_sem, axis, peer):
    return pltpu.make_async_remote_copy(
        src_ref=src,
        dst_ref=dst,
        send_sem=send_sem,
        recv_sem=recv_sem,
        device_id={axis: peer},
        device_id_type=pl.DeviceIdType.MESH,
    )


def attend(s, length, query_ref, ck_ref, cv_ref, att_ref, kv_count):
    _, heads, size = query_ref.shape
    span = ck_ref.shape[1]
    column = lax.broadcasted_iota(I32, (heads, span), 1)
    row = lax.broadcasted_iota(I32, (heads, span), 0)
    own = lax.rem(column, kv_count) == row // (heads // kv_count)
    scores = lax.dot_general(
        query_ref[s], ck_ref[s], (((1,), (1,)), ((), ())),
        preferred_element_type=F32,
    ) * size ** (-0.5)
    live = own & (column < length * kv_count)
    masked = jnp.where(live, scores, -jnp.inf)
    peak = jnp.max(masked, axis=1, keepdims=True)
    weighted = jnp.exp(masked - peak)
    prob = (weighted / jnp.sum(weighted, axis=1, keepdims=True)).astype(BF16)
    att_ref[s] = jnp.dot(prob, cv_ref[s], preferred_element_type=F32).astype(BF16)


def moe_kernel(
    n_attn,
    n_exp,
    experts,
    kv_count,
    tok_hbm,
    ids_hbm,
    gw_hbm,
    wg_hbm,
    wu_hbm,
    wd_hbm,
    length_hbm,
    query_hbm,
    ck_hbm,
    cv_hbm,
    out_hbm,
    att_hbm,
    out_ref,
    att_ref,
    wg,
    wu,
    wd,
    ck,
    cv,
    query,
    length,
    tok_all,
    ids_all,
    gw_all,
    pos,
    gate_of,
    part,
    part_in,
    hid,
    acc,
    final,
    early,
    res,
    ret1,
    ret1_in,
    ret2,
    ret2_in,
    w_sem,
    c_sem,
    out_sem,
    ids_s,
    ids_r,
    gw_s,
    gw_r,
    far_s,
    far_r,
    near_s,
    near_r,
    part_s,
    part_r,
    hid_s,
    hid_r,
    ret1_s,
    ret1_r,
    ret2_s,
    ret2_r,
):
    me = lax.axis_index("attn")
    mine = lax.axis_index("expert")
    lane = lax.rem(me, 2)
    line = me // 2
    lines = n_attn // 2
    partner = me + 1 - 2 * lane
    last = n_exp - 1
    local = wg.shape[0]
    rows, feat = tok_all.shape[1:]
    ffn = wg.shape[2]
    feat_out = wd.shape[2]
    topk = ids_all.shape[1]
    half = part.shape[2]
    capacity = 2 * half
    all_rows = n_attn * rows
    per = half // CHUNK_ROWS
    chunks = local * per
    cut = feat // TOKEN_CUTS
    out_cut = feat_out // RETURN_CUTS

    def at_line(other):
        return lax.rem(other + 2 * lines, lines)

    tok_copy = pltpu.make_async_copy(tok_hbm, tok_all.at[lines + line], c_sem.at[0])
    ids_copy = pltpu.make_async_copy(ids_hbm, ids_all.at[me], c_sem.at[1])
    gw_copy = pltpu.make_async_copy(gw_hbm, gw_all.at[me], c_sem.at[2])
    len_copy = pltpu.make_async_copy(length_hbm, length, c_sem.at[3])
    query_copy = pltpu.make_async_copy(query_hbm, query, c_sem.at[4])
    ck_copy = pltpu.make_async_copy(ck_hbm, ck, c_sem.at[5])
    cv_copy = pltpu.make_async_copy(cv_hbm, cv, c_sem.at[6])
    for copy in (ids_copy, gw_copy, tok_copy):
        copy.start()

    barrier = pltpu.get_barrier_semaphore()
    for d in range(1, n_attn):
        pl.semaphore_signal(
            barrier, inc=1, device_id={"attn": lax.rem(me + d, n_attn)},
            device_id_type=pl.DeviceIdType.MESH,
        )

    @pl.when(mine > 0)
    def _():
        pl.semaphore_signal(
            barrier, inc=1, device_id={"expert": mine - 1},
            device_id_type=pl.DeviceIdType.MESH,
        )

    @pl.when(mine < last)
    def _():
        pl.semaphore_signal(
            barrier, inc=1, device_id={"expert": mine + 1},
            device_id_type=pl.DeviceIdType.MESH,
        )

    ends = jnp.where(mine > 0, 1, 0) + jnp.where(mine < last, 1, 0)
    ids_copy.wait()
    gw_copy.wait()
    tok_copy.wait()
    for copy in (query_copy, len_copy, ck_copy, cv_copy):
        copy.start()

    def weight_copy(i, j):
        src, dst = ((wg_hbm, wg), (wu_hbm, wu), (wd_hbm, wd))[i]
        return pltpu.make_async_copy(src.at[j], dst.at[j], w_sem.at[i, j])

    for j in range(local):
        weight_copy(0, j).start()
        weight_copy(1, j).start()
    for j in range(local):
        weight_copy(2, j).start()

    pl.semaphore_wait(barrier, n_attn - 1 + ends)

    def ids_send(d, slot):
        return remote(ids_all.at[slot], ids_all.at[slot], ids_s.at[d - 1], ids_r.at[d - 1],
                      "attn", lax.rem(me + d, n_attn))

    def gw_send(d, slot):
        return remote(gw_all.at[slot], gw_all.at[slot], gw_s.at[d - 1], gw_r.at[d - 1],
                      "attn", lax.rem(me + d, n_attn))

    def far(d, q, block):
        view = tok_all.at[lines + block, :, pl.ds(q * cut, cut)]
        return remote(view, view, far_s.at[d - 1, q], far_r.at[d - 1, q],
                      "attn", at_line(line + d) * 2 + lane)

    def near(d, q):
        block = at_line(line - d)
        columns = pl.ds(q * cut, cut)
        return remote(tok_all.at[lines + block, :, columns], tok_all.at[block, :, columns],
                      near_s.at[d, q], near_r.at[d, q], "attn", partner)

    for d in range(1, n_attn):
        ids_send(d, me).start()
        gw_send(d, me).start()
    for q in range(TOKEN_CUTS):
        for d in range(1, lines):
            far(d, q, line).start()
    for q in range(TOKEN_CUTS):
        near(0, q).start()

    acc[...] = jnp.zeros_like(acc)

    for d in range(1, n_attn):
        ids_send(d, lax.rem(me + n_attn - d, n_attn)).wait_recv()
        gw_send(d, lax.rem(me + n_attn - d, n_attn)).wait_recv()

    before = (
        lax.broadcasted_iota(I32, (rows, rows), 0)
        < lax.broadcasted_iota(I32, (rows, rows), 1)
    ).astype(F32).astype(BF16)
    names = lax.broadcasted_iota(I32, (experts, rows), 0)
    offset = jnp.zeros((experts, 1), F32)
    for b in range(n_attn):
        member = jnp.zeros((experts, rows), F32)
        factor = jnp.zeros((experts, rows), F32)
        wide = gw_all[b].astype(F32)
        for k in range(topk):
            hit = names == ids_all[b, k:k + 1, :]
            member = jnp.where(hit, 1.0, member)
            factor = jnp.where(hit, wide[k:k + 1, :], factor)
        place = jnp.dot(member.astype(BF16), before, preferred_element_type=F32) + offset
        offset = offset + jnp.sum(member, axis=1, keepdims=True)
        here = lax.rem(b + lane + 1, 2) * lines + b // 2
        columns = pl.ds(pl.multiple_of(here * rows, rows), rows)
        pos[:, columns] = jnp.where(member > 0.5, place, -1.0).astype(I32)
        gate_of[:, columns] = factor

    len_copy.wait()
    query_copy.wait()
    ck_copy.wait()
    cv_copy.wait()
    def relay(q):
        for d in range(1, lines):
            far(d, q, at_line(line - d)).wait_recv()
            near(d, q).start()

    def chosen_of(j):
        place = pos[pl.ds(me * local + j, 1), :]
        slots = lax.broadcasted_iota(I32, (capacity, all_rows), 0)
        return (slots == place).astype(F32).astype(BF16)

    def start_first(q):
        for d in range(lines):
            near(d, q).wait_recv()
        columns = slice(q * cut, (q + 1) * cut)
        packed = jnp.dot(
            final[...], tok_all[:, :, columns].reshape(all_rows, cut),
            preferred_element_type=F32,
        ).astype(BF16)
        for w, to in ((wg, 0), (wu, ffn)):
            term = jnp.dot(packed, w[0, columns, :], preferred_element_type=F32)
            if q > 0:
                term = term + early[:, to:to + ffn]
            if q < TOKEN_CUTS - 1:
                early[:, to:to + ffn] = term
            else:
                part[0, :, :, to:to + ffn] = term.astype(BF16).reshape(2, half, ffn)

    final[...] = chosen_of(0)
    seqs = query.shape[0]
    for q in range(TOKEN_CUTS):
        relay(q)
        for s in range(seqs):
            if s * (TOKEN_CUTS - 1) // seqs == q:
                attend(s, length[s], query, ck, cv, att_ref, kv_count)
        if q == TOKEN_CUTS - 2:
            weight_copy(0, 0).wait()
            weight_copy(1, 0).wait()
            for r in range(q):
                start_first(r)
    for q in range(max(TOKEN_CUTS - 2, 0), TOKEN_CUTS):
        start_first(q)

    att_copy = pltpu.make_async_copy(att_ref, att_hbm, c_sem.at[7])
    att_copy.start()

    def steps_from(way):
        return mine if way == 0 else last - mine

    def piece(ref, way, k):
        j = k // per
        first_row = pl.multiple_of(lax.rem(k, per) * CHUNK_ROWS, CHUNK_ROWS)
        return ref.at[j, way, pl.ds(first_row, CHUNK_ROWS)]

    def part_copy(way, k):
        return remote(piece(part, way, k), piece(part_in, way, k),
                      part_s.at[way, k // per], part_r.at[way, k],
                      "expert", lax.rem(mine + 1 - 2 * way + n_exp, n_exp))

    def hid_copy(way, k):
        return remote(piece(hid, way, k), piece(hid, way, k),
                      hid_s.at[way, k // per], hid_r.at[way, k],
                      "expert", lax.rem(mine - 1 + 2 * way + n_exp, n_exp))

    def send_parts(j):
        for way in range(2):
            @pl.when(steps_from(way) == 0)
            def _():
                for r in range(per):
                    part_copy(way, j * per + r).start()

    def first(j, carry):
        packed = jnp.dot(
            chosen_of(j), tok_all[...].reshape(all_rows, feat),
            preferred_element_type=F32,
        ).astype(BF16)
        weight_copy(0, j).wait()
        weight_copy(1, j).wait()
        gate = jnp.dot(packed, wg[j], preferred_element_type=F32).astype(BF16)
        part[j, :, :, :ffn] = gate.reshape(2, half, ffn)
        up = jnp.dot(packed, wu[j], preferred_element_type=F32).astype(BF16)
        part[j, :, :, ffn:] = up.reshape(2, half, ffn)
        send_parts(j)
        return carry

    send_parts(0)
    lax.fori_loop(1, local - 1, first, 0)

    def reduce(way, k):
        part_copy(way, k).wait_recv()
        total = piece(part, way, k)[...].astype(F32) + piece(part_in, way, k)[...].astype(F32)

        @pl.when(steps_from(way) < last)
        def _():
            piece(part, way, k)[...] = total.astype(BF16)
            part_copy(way, k).start()

        @pl.when(steps_from(way) == last)
        def _():
            gate = total[:, :ffn]
            piece(hid, way, k)[...] = (
                gate / (1.0 + jnp.exp(-gate)) * total[:, ffn:]
            ).astype(BF16)
            hid_copy(way, k).start()

    def reduce_step(s, carry):
        for way in range(2):
            k = s - LAG * (steps_from(way) - 1)

            @pl.when((steps_from(way) > 0) & (k >= 0) & (k < chunks))
            def _():
                reduce(way, k)
        return carry

    def pass_on(s, carry):
        for way in range(2):
            hops = last - steps_from(way)
            k = s - HLAG * (hops - 1)
            due = (hops > 0) & (k >= 0) & (k < chunks)

            @pl.when(due)
            def _():
                hid_copy(way, k).wait_recv()

            @pl.when(due & (hops < last))
            def _():
                hid_copy(way, k).start()
        return carry

    ahead = HLAG * (last - 1)
    over = LAG * (last - 1)

    def both_steps(s, carry):
        reduce_step(s, carry)
        for i in range(PACE):
            pass_on((s - chunks) * PACE + i, carry)
        return carry

    lax.fori_loop(0, FIRST_STEPS, reduce_step, 0)
    first(local - 1, 0)
    lax.fori_loop(FIRST_STEPS, chunks, reduce_step, 0)
    lax.fori_loop(chunks, chunks + over, both_steps, 0)
    lax.fori_loop(min(over * PACE, ahead), ahead, pass_on, 0)

    def spread_of(j):
        place = pos[pl.ds(me * local + j, 1), :]
        factor = gate_of[pl.ds(me * local + j, 1), :]
        slots = lax.broadcasted_iota(I32, (capacity, all_rows), 0)
        return jnp.where(slots == place, factor, 0.0).astype(BF16)

    def combine(spread, result):
        return lax.dot_general(
            spread, result, (((0,), (0,)), ((), ())), preferred_element_type=F32
        )

    def second(j, carry):
        lax.fori_loop(jnp.maximum(ahead + j * per, over * PACE), ahead + (j + 1) * per, pass_on, 0)
        weight_copy(2, j).wait()
        result = jnp.dot(
            hid[j].reshape(capacity, ffn), wd[j], preferred_element_type=F32
        ).astype(BF16)
        acc[...] += combine(spread_of(j), result)
        return carry

    lax.fori_loop(0, local - 1, second, 0)
    j = local - 1
    weight_copy(2, j).wait()
    final[...] = spread_of(j)
    lax.fori_loop(ahead + j * per, ahead + (j + 1) * per, pass_on, 0)

    split = all_rows // 2

    def ret1_copy(q):
        columns = pl.ds(q * out_cut, out_cut)
        return remote(ret1.at[:, columns], ret1_in.at[:, columns],
                      ret1_s.at[q], ret1_r.at[q], "attn", partner)

    def ret2_copy(d, q):
        columns = pl.ds(q * out_cut, out_cut)
        return remote(ret2.at[d - 1, :, columns], ret2_in.at[d - 1, :, columns],
                      ret2_s.at[d - 1, q], ret2_r.at[d - 1, q],
                      "attn", at_line(line + d) * 2 + lane)

    def columns_of(q):
        return slice(q * out_cut, (q + 1) * out_cut)

    def own(index, q):
        return pl.ds(pl.multiple_of(split + index * rows, rows), rows), columns_of(q)

    def got(index, q):
        return pl.ds(pl.multiple_of(index * rows, rows), rows), columns_of(q)

    def to_partner(q):
        columns = columns_of(q)
        result = jnp.dot(
            hid[j].reshape(capacity, ffn), wd[j, :, columns], preferred_element_type=F32
        ).astype(BF16)
        res[:, columns] = result
        ret1[:, columns] = (acc[:split, columns] + combine(final[:, :split], result)).astype(BF16)
        ret1_copy(q).start()

    def to_lines(q):
        columns = columns_of(q)
        acc[split:, columns] += combine(final[:, split:], res[:, columns])
        ret1_copy(q).wait_recv()
        for d in range(1, lines):
            to = at_line(line + d)
            ret2[d - 1, :, columns] = (
                acc[own(to, q)] + ret1_in[got(to, q)].astype(F32)
            ).astype(BF16)
            ret2_copy(d, q).start()

    for q in range(RETURN_CUTS):
        to_partner(q)
        if q >= RETURN_DELAY:
            to_lines(q - RETURN_DELAY)
    for q in range(max(RETURN_CUTS - RETURN_DELAY, 0), RETURN_CUTS):
        to_lines(q)
    def out_copy(q):
        columns = pl.ds(q * out_cut, out_cut)
        return pltpu.make_async_copy(out_ref.at[:, columns], out_hbm.at[:, columns], out_sem.at[q])

    for q in range(RETURN_CUTS):
        total = acc[own(line, q)] + ret1_in[got(line, q)].astype(F32)
        for d in range(1, lines):
            ret2_copy(d, q).wait_recv()
            total = total + ret2_in[d - 1, :, columns_of(q)].astype(F32)
        out_ref[:, columns_of(q)] = total.astype(BF16)
        out_copy(q).start()

    for d in range(1, n_attn):
        ids_send(d, me).wait_send()
        gw_send(d, me).wait_send()
    for q in range(TOKEN_CUTS):
        near(0, q).wait_send()
        for d in range(1, lines):
            far(d, q, line).wait_send()
            near(d, q).wait_send()
    for q in range(RETURN_CUTS):
        ret1_copy(q).wait_send()
        for d in range(1, lines):
            ret2_copy(d, q).wait_send()

    att_copy.wait()
    for q in range(RETURN_CUTS):
        out_copy(q).wait()

    for way in range(2):
        for j in range(local):
            @pl.when(steps_from(way) < last)
            def _():
                remote(part.at[j, way], part_in.at[j, way], part_s.at[way, j], part_r.at[way, 0],
                       "expert", lax.rem(mine + 1 - 2 * way + n_exp, n_exp)).wait_send()

            @pl.when(steps_from(way) > 0)
            def _():
                remote(hid.at[j, way], hid.at[j, way], hid_s.at[way, j], hid_r.at[way, 0],
                       "expert", lax.rem(mine - 1 + 2 * way + n_exp, n_exp)).wait_send()


def routed(tokens, expert_ids, gate_weight, w_gate, w_up, w_down, query, cache_k, cache_v, lengths, n_attn, n_exp):
    rows, feat = tokens.shape
    local, _, ffn = w_gate.shape
    feat_out = w_down.shape[2]
    topk = expert_ids.shape[1]
    experts = local * n_attn
    capacity = rows * topk // local
    half = capacity // 2
    lines = n_attn // 2
    chunks = local * (half // CHUNK_ROWS)
    seqs, heads, size = query.shape
    context, kv_count = cache_k.shape[1:3]
    flat = (seqs, context * kv_count, size)
    dma = pltpu.SemaphoreType.DMA
    vmem = pltpu.VMEM
    return pl.pallas_call(
        functools.partial(moe_kernel, n_attn, n_exp, experts, kv_count),
        out_shape=(
            jax.ShapeDtypeStruct((rows, feat_out), BF16),
            jax.ShapeDtypeStruct(query.shape, BF16),
        ),
        in_specs=[pl.BlockSpec(memory_space=pltpu.HBM)] * 10,
        out_specs=[pl.BlockSpec(memory_space=pltpu.HBM)] * 2,
        scratch_shapes=[
            vmem((rows, feat_out), BF16),
            vmem(query.shape, BF16),
            vmem(w_gate.shape, BF16),
            vmem(w_up.shape, BF16),
            vmem(w_down.shape, BF16),
            vmem(flat, BF16),
            vmem(flat, BF16),
            vmem(query.shape, BF16),
            pltpu.SMEM(lengths.shape, I32),
            vmem((n_attn, rows, feat), BF16),
            vmem((n_attn, topk, rows), I32),
            vmem((n_attn, topk, rows), BF16),
            vmem((experts, n_attn * rows), I32),
            vmem((experts, n_attn * rows), F32),
            vmem((local, 2, half, 2 * ffn), BF16),
            vmem((local, 2, half, 2 * ffn), BF16),
            vmem((local, 2, half, ffn), BF16),
            vmem((n_attn * rows, feat_out), F32),
            vmem((capacity, n_attn * rows), BF16),
            vmem((capacity, 2 * ffn), F32),
            vmem((capacity, feat_out), BF16),
            vmem((lines * rows, feat_out), BF16),
            vmem((lines * rows, feat_out), BF16),
            vmem((lines - 1, rows, feat_out), BF16),
            vmem((lines - 1, rows, feat_out), BF16),
            dma((3, local)),
            dma((8,)),
            dma((RETURN_CUTS,)),
            dma((n_attn - 1,)),
            dma((n_attn - 1,)),
            dma((n_attn - 1,)),
            dma((n_attn - 1,)),
            dma((lines - 1, TOKEN_CUTS)),
            dma((lines - 1, TOKEN_CUTS)),
            dma((lines, TOKEN_CUTS)),
            dma((lines, TOKEN_CUTS)),
            dma((2, local)),
            dma((2, chunks)),
            dma((2, local)),
            dma((2, chunks)),
            dma((RETURN_CUTS,)),
            dma((RETURN_CUTS,)),
            dma((lines - 1, RETURN_CUTS)),
            dma((lines - 1, RETURN_CUTS)),
        ],
        compiler_params=pltpu.CompilerParams(
            collective_id=0, has_side_effects=True, vmem_limit_bytes=56 * 1024 * 1024
        ),
    )(
        tokens, expert_ids.T, gate_weight.T, w_gate, w_up, w_down, lengths, query,
        cache_k.reshape(flat), cache_v.reshape(flat),
    )


def finish_kernel(moe_ref, att_ref, out_ref, attn_out_ref):
    heads, size = att_ref.shape[1:]
    out_ref[...] = moe_ref[...]
    for h in range(heads):
        attn_out_ref[:, h * size:(h + 1) * size] = att_ref[:, h, :]


def finish(moe, att):
    seqs, heads, size = att.shape
    return pl.pallas_call(
        finish_kernel,
        out_shape=(
            jax.ShapeDtypeStruct(moe.shape, moe.dtype),
            jax.ShapeDtypeStruct((seqs, heads * size), att.dtype),
        ),
        in_specs=[pl.BlockSpec(memory_space=pltpu.VMEM)] * 2,
        out_specs=[pl.BlockSpec(memory_space=pltpu.VMEM)] * 2,
    )(moe, att)


def body(tokens, expert_ids, gate_weight, w_gate, w_up, w_down, query, cache_k, cache_v, lengths):
    n_attn = lax.axis_size("attn")
    n_exp = lax.axis_size("expert")
    moe_out, attended = routed(
        tokens, expert_ids, gate_weight, w_gate, w_up, w_down,
        query, cache_k, cache_v, lengths, n_attn, n_exp,
    )
    return finish(moe_out, attended)


def solution(mesh):
    return jax.shard_map(
        body,
        mesh=mesh,
        in_specs=(
            P(("groups", "attn"), "expert"),
            P(("groups", "attn"), None),
            P(("groups", "attn"), None),
            P("attn", "expert", None),
            P("attn", "expert", None),
            P("attn", None, "expert"),
            P(("groups", "attn", "expert"), None, None),
            P(("groups", "attn", "expert"), None, None, None),
            P(("groups", "attn", "expert"), None, None, None),
            P(("groups", "attn", "expert")),
        ),
        out_specs=(P(("groups", "attn"), "expert"), P(("groups", "attn", "expert"), None)),
        check_vma=False,
    )
```

```python
import functools

import jax
import jax.numpy as jnp
from jax import lax
from jax.experimental import pallas as pl
from jax.experimental.pallas import tpu as pltpu
from jax.sharding import PartitionSpec as P

F32 = jnp.float32
BF16 = jnp.bfloat16
I32 = jnp.int32

TOKEN_CUTS = 4
CHUNK_ROWS = 16
LAG = 3
HLAG = 8
PACE = 2
RETURN_CUTS = 4
RETURN_DELAY = 2


def remote(src, dst, send_sem, recv_sem, axis, peer):
    return pltpu.make_async_remote_copy(
        src_ref=src,
        dst_ref=dst,
        send_sem=send_sem,
        recv_sem=recv_sem,
        device_id={axis: peer},
        device_id_type=pl.DeviceIdType.MESH,
    )


def attend(s, length, query_ref, ck_ref, cv_ref, att_ref, kv_count):
    _, heads, size = query_ref.shape
    span = ck_ref.shape[1]
    column = lax.broadcasted_iota(I32, (heads, span), 1)
    row = lax.broadcasted_iota(I32, (heads, span), 0)
    own = lax.rem(column, kv_count) == row // (heads // kv_count)
    scores = lax.dot_general(
        query_ref[s], ck_ref[s], (((1,), (1,)), ((), ())),
        preferred_element_type=F32,
    ) * size ** (-0.5)
    live = own & (column < length * kv_count)
    masked = jnp.where(live, scores, -jnp.inf)
    peak = jnp.max(masked, axis=1, keepdims=True)
    weighted = jnp.exp(masked - peak)
    prob = (weighted / jnp.sum(weighted, axis=1, keepdims=True)).astype(BF16)
    att_ref[s] = jnp.dot(prob, cv_ref[s], preferred_element_type=F32).astype(BF16)


def moe_kernel(
    n_attn,
    n_exp,
    experts,
    kv_count,
    tok_hbm,
    ids_hbm,
    gw_hbm,
    wg_hbm,
    wu_hbm,
    wd_hbm,
    length_hbm,
    query_hbm,
    ck_hbm,
    cv_hbm,
    out_hbm,
    att_hbm,
    out_ref,
    att_ref,
    wg,
    wu,
    wd,
    ck,
    cv,
    query,
    length,
    tok_all,
    ids_all,
    gw_all,
    pos,
    gate_of,
    part,
    part_in,
    hid,
    acc,
    chosen,
    final,
    early,
    res,
    ret1,
    ret1_in,
    ret2,
    ret2_in,
    w_sem,
    c_sem,
    out_sem,
    ids_s,
    ids_r,
    gw_s,
    gw_r,
    far_s,
    far_r,
    near_s,
    near_r,
    part_s,
    part_r,
    hid_s,
    ret1_s,
    ret1_r,
    ret2_s,
    ret2_r,
):
    me = lax.axis_index("attn")
    mine = lax.axis_index("expert")
    lane = lax.rem(me, 2)
    line = me // 2
    lines = n_attn // 2
    partner = me + 1 - 2 * lane
    last = n_exp - 1
    local = wg.shape[0]
    rows, feat = tok_all.shape[1:]
    ffn = wg.shape[2]
    feat_out = wd.shape[2]
    topk = ids_all.shape[1]
    half = part.shape[2]
    capacity = 2 * half
    all_rows = n_attn * rows
    per = half // CHUNK_ROWS
    chunks = local * per
    cut = feat // TOKEN_CUTS
    out_cut = feat_out // RETURN_CUTS

    def at_line(other):
        return lax.rem(other + 2 * lines, lines)

    tok_copy = pltpu.make_async_copy(tok_hbm, tok_all.at[lines + line], c_sem.at[0])
    ids_copy = pltpu.make_async_copy(ids_hbm, ids_all.at[me], c_sem.at[1])
    gw_copy = pltpu.make_async_copy(gw_hbm, gw_all.at[me], c_sem.at[2])
    len_copy = pltpu.make_async_copy(length_hbm, length, c_sem.at[3])
    query_copy = pltpu.make_async_copy(query_hbm, query, c_sem.at[4])
    ck_copy = pltpu.make_async_copy(ck_hbm, ck, c_sem.at[5])
    cv_copy = pltpu.make_async_copy(cv_hbm, cv, c_sem.at[6])
    for copy in (ids_copy, gw_copy, tok_copy):
        copy.start()

    barrier = pltpu.get_barrier_semaphore()
    for d in range(1, n_attn):
        pl.semaphore_signal(
            barrier, inc=1, device_id={"attn": lax.rem(me + d, n_attn)},
            device_id_type=pl.DeviceIdType.MESH,
        )

    @pl.when(mine > 0)
    def _():
        pl.semaphore_signal(
            barrier, inc=1, device_id={"expert": mine - 1},
            device_id_type=pl.DeviceIdType.MESH,
        )

    @pl.when(mine < last)
    def _():
        pl.semaphore_signal(
            barrier, inc=1, device_id={"expert": mine + 1},
            device_id_type=pl.DeviceIdType.MESH,
        )

    ends = jnp.where(mine > 0, 1, 0) + jnp.where(mine < last, 1, 0)
    ids_copy.wait()
    gw_copy.wait()
    tok_copy.wait()
    for copy in (query_copy, len_copy, ck_copy, cv_copy):
        copy.start()

    def weight_copy(i, j):
        src, dst = ((wg_hbm, wg), (wu_hbm, wu), (wd_hbm, wd))[i]
        return pltpu.make_async_copy(src.at[j], dst.at[j], w_sem.at[i, j])

    for j in range(local):
        weight_copy(0, j).start()
        weight_copy(1, j).start()
    for j in range(local):
        weight_copy(2, j).start()

    pl.semaphore_wait(barrier, n_attn - 1 + ends)

    def ids_send(d, slot):
        return remote(ids_all.at[slot], ids_all.at[slot], ids_s.at[d - 1], ids_r.at[d - 1],
                      "attn", lax.rem(me + d, n_attn))

    def gw_send(d, slot):
        return remote(gw_all.at[slot], gw_all.at[slot], gw_s.at[d - 1], gw_r.at[d - 1],
                      "attn", lax.rem(me + d, n_attn))

    def far(d, q, block):
        view = tok_all.at[lines + block, :, pl.ds(q * cut, cut)]
        return remote(view, view, far_s.at[d - 1, q], far_r.at[d - 1, q],
                      "attn", at_line(line + d) * 2 + lane)

    def near(d, q):
        block = at_line(line - d)
        columns = pl.ds(q * cut, cut)
        return remote(tok_all.at[lines + block, :, columns], tok_all.at[block, :, columns],
                      near_s.at[d, q], near_r.at[d, q], "attn", partner)

    for d in range(1, n_attn):
        ids_send(d, me).start()
        gw_send(d, me).start()
    for q in range(TOKEN_CUTS):
        for d in range(1, lines):
            far(d, q, line).start()
    for q in range(TOKEN_CUTS):
        near(0, q).start()

    acc[...] = jnp.zeros_like(acc)

    for d in range(1, n_attn):
        ids_send(d, lax.rem(me + n_attn - d, n_attn)).wait_recv()
        gw_send(d, lax.rem(me + n_attn - d, n_attn)).wait_recv()

    before = (
        lax.broadcasted_iota(I32, (rows, rows), 0)
        < lax.broadcasted_iota(I32, (rows, rows), 1)
    ).astype(F32).astype(BF16)
    names = lax.broadcasted_iota(I32, (experts, rows), 0)
    offset = jnp.zeros((experts, 1), F32)
    for b in range(n_attn):
        member = jnp.zeros((experts, rows), F32)
        factor = jnp.zeros((experts, rows), F32)
        wide = gw_all[b].astype(F32)
        for k in range(topk):
            hit = names == ids_all[b, k:k + 1, :]
            member = jnp.where(hit, 1.0, member)
            factor = jnp.where(hit, wide[k:k + 1, :], factor)
        place = jnp.dot(member.astype(BF16), before, preferred_element_type=F32) + offset
        offset = offset + jnp.sum(member, axis=1, keepdims=True)
        here = lax.rem(b + lane + 1, 2) * lines + b // 2
        columns = pl.ds(pl.multiple_of(here * rows, rows), rows)
        pos[:, columns] = jnp.where(member > 0.5, place, -1.0).astype(I32)
        gate_of[:, columns] = factor

    def spread_of(j):
        place = pos[pl.ds(me * local + j, 1), :]
        factor = gate_of[pl.ds(me * local + j, 1), :]
        slots = lax.broadcasted_iota(I32, (capacity, all_rows), 0)
        return jnp.where(slots == place, factor, 0.0)

    def relay(q):
        for d in range(1, lines):
            far(d, q, at_line(line - d)).wait_recv()
            near(d, q).start()

    def chosen_of(j):
        place = pos[pl.ds(me * local + j, 1), :]
        slots = lax.broadcasted_iota(I32, (capacity, all_rows), 0)
        return (slots == place).astype(F32).astype(BF16)

    def start_first(q):
        for d in range(lines):
            near(d, q).wait_recv()
        columns = slice(q * cut, (q + 1) * cut)
        packed = jnp.dot(
            chosen[...], tok_all[:, :, columns].reshape(all_rows, cut),
            preferred_element_type=F32,
        ).astype(BF16)
        for w, to in ((wg, 0), (wu, ffn)):
            term = jnp.dot(packed, w[0, columns, :], preferred_element_type=F32)
            if q > 0:
                term = term + early[:, to:to + ffn]
            if q < TOKEN_CUTS - 1:
                early[:, to:to + ffn] = term
            else:
                part[0, :, :, to:to + ffn] = term.astype(BF16).reshape(2, half, ffn)

    chosen[...] = chosen_of(0)
    final[...] = spread_of(local - 1).T.astype(BF16)
    relay(0)
    weight_copy(0, 0).wait()
    weight_copy(1, 0).wait()
    for q in range(1, TOKEN_CUTS):
        relay(q)
        start_first(q - 1)
    start_first(TOKEN_CUTS - 1)

    def steps_from(way):
        return mine + way * (last - 2 * mine)

    near_way = 2 * mine // n_exp

    def piece(ref, way, k):
        j = k // per
        first_row = pl.multiple_of(lax.rem(k, per) * CHUNK_ROWS, CHUNK_ROWS)
        return ref.at[j, way, pl.ds(first_row, CHUNK_ROWS)]

    def part_copy(way, k):
        return remote(piece(part, way, k), piece(part_in, way, k),
                      part_s.at[way, k // per], part_r.at[way, k],
                      "expert", lax.rem(mine + 1 - 2 * way + n_exp, n_exp))

    def hid_copy(way, k):
        return remote(piece(hid, way, k), piece(hid, way, k),
                      hid_s.at[way, k // per], part_r.at[way, k],
                      "expert", lax.rem(mine - 1 + 2 * way + n_exp, n_exp))

    def send_parts(j):
        for way in range(2):
            @pl.when(steps_from(way) == 0)
            def _():
                for r in range(per):
                    part_copy(way, j * per + r).start()

    def first(j, carry):
        packed = jnp.dot(
            chosen_of(j), tok_all[...].reshape(all_rows, feat),
            preferred_element_type=F32,
        ).astype(BF16)
        weight_copy(0, j).wait()
        weight_copy(1, j).wait()
        gate = jnp.dot(packed, wg[j], preferred_element_type=F32).astype(BF16)
        part[j, :, :, :ffn] = gate.reshape(2, half, ffn)
        up = jnp.dot(packed, wu[j], preferred_element_type=F32).astype(BF16)
        part[j, :, :, ffn:] = up.reshape(2, half, ffn)
        send_parts(j)
        return carry

    send_parts(0)
    lax.fori_loop(1, local, first, 0)

    def reduce(way, k):
        part_copy(way, k).wait_recv()
        total = piece(part, way, k)[...].astype(F32) + piece(part_in, way, k)[...].astype(F32)

        @pl.when(steps_from(way) < last)
        def _():
            piece(part, way, k)[...] = total.astype(BF16)
            part_copy(way, k).start()

        @pl.when(steps_from(way) == last)
        def _():
            gate = total[:, :ffn]
            piece(hid, way, k)[...] = (
                gate / (1.0 + jnp.exp(-gate)) * total[:, ffn:]
            ).astype(BF16)
            hid_copy(way, k).start()

    def reduce_step(s, carry):
        for way in (near_way, 1 - near_way):
            k = s - LAG * (steps_from(way) - 1)

            @pl.when((steps_from(way) > 0) & (k >= 0) & (k < chunks))
            def _():
                reduce(way, k)
        return carry

    def pass_on(s, carry):
        for way in (1 - near_way, near_way):
            hops = last - steps_from(way)
            k = s - HLAG * (hops - 1)
            due = (hops > 0) & (k >= 0) & (k < chunks)

            @pl.when(due)
            def _():
                hid_copy(way, k).wait_recv()

            @pl.when(due & (hops < last))
            def _():
                hid_copy(way, k).start()
        return carry

    ahead = HLAG * (last - 1)
    over = LAG * (last - 1)

    def both_steps(s, carry):
        reduce_step(s, carry)
        for i in range(PACE):
            pass_on((s - chunks) * PACE + i, carry)
        return carry

    lax.fori_loop(0, chunks, reduce_step, 0)
    lax.fori_loop(chunks, chunks + over, both_steps, 0)
    lax.fori_loop(min(over * PACE, ahead), ahead, pass_on, 0)

    def combine(spread, result):
        return lax.dot_general(
            spread, result, (((0,), (0,)), ((), ())), preferred_element_type=F32
        )

    def second(j, carry):
        lax.fori_loop(jnp.maximum(ahead + j * per, over * PACE), ahead + (j + 1) * per, pass_on, 0)
        weight_copy(2, j).wait()
        result = jnp.dot(
            hid[j].reshape(capacity, ffn), wd[j], preferred_element_type=F32
        ).astype(BF16)
        acc[...] += combine(spread_of(j).astype(BF16), result)
        return carry

    lax.fori_loop(0, local - 1, second, 0)
    j = local - 1
    weight_copy(2, j).wait()
    lax.fori_loop(ahead + j * per, ahead + (j + 1) * per, pass_on, 0)

    split = all_rows // 2

    def ret1_copy(q):
        columns = pl.ds(q * out_cut, out_cut)
        return remote(ret1.at[:, columns], ret1_in.at[:, columns],
                      ret1_s.at[q], ret1_r.at[q], "attn", partner)

    def ret2_copy(d, q):
        columns = pl.ds(q * out_cut, out_cut)
        return remote(ret2.at[d - 1, :, columns], ret2_in.at[d - 1, :, columns],
                      ret2_s.at[d - 1, q], ret2_r.at[d - 1, q],
                      "attn", at_line(line + d) * 2 + lane)

    def columns_of(q):
        return slice(q * out_cut, (q + 1) * out_cut)

    def own(index, q):
        return pl.ds(pl.multiple_of(split + index * rows, rows), rows), columns_of(q)

    def got(index, q):
        return pl.ds(pl.multiple_of(index * rows, rows), rows), columns_of(q)

    def to_partner(q):
        columns = columns_of(q)
        result = jnp.dot(
            hid[j].reshape(capacity, ffn), wd[j, :, columns], preferred_element_type=F32
        ).astype(BF16)
        res[:, columns] = result
        ret1[:, columns] = (acc[:split, columns] + jnp.dot(final[:split], result, preferred_element_type=F32)).astype(BF16)
        ret1_copy(q).start()

    def to_lines(q):
        columns = columns_of(q)
        acc[split:, columns] += jnp.dot(
            final[split:], res[:, columns], preferred_element_type=F32
        )
        ret1_copy(q).wait_recv()
        for d in range(1, lines):
            to = at_line(line + d)
            ret2[d - 1, :, columns] = (
                acc[own(to, q)] + ret1_in[got(to, q)].astype(F32)
            ).astype(BF16)
            ret2_copy(d, q).start()

    for q in range(RETURN_CUTS):
        to_partner(q)
        if q >= RETURN_DELAY:
            to_lines(q - RETURN_DELAY)
    for q in range(max(RETURN_CUTS - RETURN_DELAY, 0), RETURN_CUTS):
        to_lines(q)
    att_copy = pltpu.make_async_copy(att_ref, att_hbm, c_sem.at[7])
    for copy in (len_copy, query_copy, ck_copy, cv_copy):
        copy.wait()
    for s in range(query.shape[0]):
        attend(s, length[s], query, ck, cv, att_ref, kv_count)
    att_copy.start()

    def out_copy(q):
        columns = pl.ds(q * out_cut, out_cut)
        return pltpu.make_async_copy(out_ref.at[:, columns], out_hbm.at[:, columns], out_sem.at[q])

    for q in range(RETURN_CUTS):
        total = acc[own(line, q)] + ret1_in[got(line, q)].astype(F32)
        for d in range(1, lines):
            ret2_copy(d, q).wait_recv()
            total = total + ret2_in[d - 1, :, columns_of(q)].astype(F32)
        out_ref[:, columns_of(q)] = total.astype(BF16)
        out_copy(q).start()

    for d in range(1, n_attn):
        ids_send(d, me).wait_send()
        gw_send(d, me).wait_send()
    for q in range(TOKEN_CUTS):
        near(0, q).wait_send()
        for d in range(1, lines):
            far(d, q, line).wait_send()
            near(d, q).wait_send()
    for q in range(RETURN_CUTS):
        ret1_copy(q).wait_send()
        for d in range(1, lines):
            ret2_copy(d, q).wait_send()

    att_copy.wait()
    for q in range(RETURN_CUTS):
        out_copy(q).wait()

    for way in range(2):
        for j in range(local):
            @pl.when(steps_from(way) < last)
            def _():
                remote(part.at[j, way], part_in.at[j, way], part_s.at[way, j], part_r.at[way, 0],
                       "expert", lax.rem(mine + 1 - 2 * way + n_exp, n_exp)).wait_send()

            @pl.when(steps_from(way) > 0)
            def _():
                remote(hid.at[j, way], hid.at[j, way], hid_s.at[way, j], part_r.at[way, 0],
                       "expert", lax.rem(mine - 1 + 2 * way + n_exp, n_exp)).wait_send()


def routed(tokens, expert_ids, gate_weight, w_gate, w_up, w_down, query, cache_k, cache_v, lengths, n_attn, n_exp):
    rows, feat = tokens.shape
    local, _, ffn = w_gate.shape
    feat_out = w_down.shape[2]
    topk = expert_ids.shape[1]
    experts = local * n_attn
    capacity = rows * topk // local
    half = capacity // 2
    lines = n_attn // 2
    chunks = local * (half // CHUNK_ROWS)
    seqs, heads, size = query.shape
    context, kv_count = cache_k.shape[1:3]
    flat = (seqs, context * kv_count, size)
    dma = pltpu.SemaphoreType.DMA
    vmem = pltpu.VMEM
    return pl.pallas_call(
        functools.partial(moe_kernel, n_attn, n_exp, experts, kv_count),
        out_shape=(
            jax.ShapeDtypeStruct((rows, feat_out), BF16),
            jax.ShapeDtypeStruct(query.shape, BF16),
        ),
        in_specs=[pl.BlockSpec(memory_space=pltpu.HBM)] * 10,
        out_specs=[pl.BlockSpec(memory_space=pltpu.HBM)] * 2,
        scratch_shapes=[
            vmem((rows, feat_out), BF16),
            vmem(query.shape, BF16),
            vmem(w_gate.shape, BF16),
            vmem(w_up.shape, BF16),
            vmem(w_down.shape, BF16),
            vmem(flat, BF16),
            vmem(flat, BF16),
            vmem(query.shape, BF16),
            pltpu.SMEM(lengths.shape, I32),
            vmem((n_attn, rows, feat), BF16),
            vmem((n_attn, topk, rows), I32),
            vmem((n_attn, topk, rows), BF16),
            vmem((experts, n_attn * rows), I32),
            vmem((experts, n_attn * rows), F32),
            vmem((local, 2, half, 2 * ffn), BF16),
            vmem((local, 2, half, 2 * ffn), BF16),
            vmem((local, 2, half, ffn), BF16),
            vmem((n_attn * rows, feat_out), F32),
            vmem((capacity, n_attn * rows), BF16),
            vmem((n_attn * rows, capacity), BF16),
            vmem((capacity, 2 * ffn), F32),
            vmem((capacity, feat_out), BF16),
            vmem((lines * rows, feat_out), BF16),
            vmem((lines * rows, feat_out), BF16),
            vmem((lines - 1, rows, feat_out), BF16),
            vmem((lines - 1, rows, feat_out), BF16),
            dma((3, local)),
            dma((8,)),
            dma((RETURN_CUTS,)),
            dma((n_attn - 1,)),
            dma((n_attn - 1,)),
            dma((n_attn - 1,)),
            dma((n_attn - 1,)),
            dma((lines - 1, TOKEN_CUTS)),
            dma((lines - 1, TOKEN_CUTS)),
            dma((lines, TOKEN_CUTS)),
            dma((lines, TOKEN_CUTS)),
            dma((2, local)),
            dma((2, chunks)),
            dma((2, local)),
            dma((RETURN_CUTS,)),
            dma((RETURN_CUTS,)),
            dma((lines - 1, RETURN_CUTS)),
            dma((lines - 1, RETURN_CUTS)),
        ],
        compiler_params=pltpu.CompilerParams(
            collective_id=0, has_side_effects=True, vmem_limit_bytes=56 * 1024 * 1024
        ),
    )(
        tokens, expert_ids.T, gate_weight.T, w_gate, w_up, w_down, lengths, query,
        cache_k.reshape(flat), cache_v.reshape(flat),
    )


def finish_kernel(moe_ref, att_ref, out_ref, attn_out_ref):
    heads, size = att_ref.shape[1:]
    out_ref[...] = moe_ref[...]
    for h in range(heads):
        attn_out_ref[:, h * size:(h + 1) * size] = att_ref[:, h, :]


def finish(moe, att):
    seqs, heads, size = att.shape
    return pl.pallas_call(
        finish_kernel,
        out_shape=(
            jax.ShapeDtypeStruct(moe.shape, moe.dtype),
            jax.ShapeDtypeStruct((seqs, heads * size), att.dtype),
        ),
        in_specs=[pl.BlockSpec(memory_space=pltpu.VMEM)] * 2,
        out_specs=[pl.BlockSpec(memory_space=pltpu.VMEM)] * 2,
    )(moe, att)


def body(tokens, expert_ids, gate_weight, w_gate, w_up, w_down, query, cache_k, cache_v, lengths):
    n_attn = lax.axis_size("attn")
    n_exp = lax.axis_size("expert")
    moe_out, attended = routed(
        tokens, expert_ids, gate_weight, w_gate, w_up, w_down,
        query, cache_k, cache_v, lengths, n_attn, n_exp,
    )
    return finish(moe_out, attended)


def solution(mesh):
    return jax.shard_map(
        body,
        mesh=mesh,
        in_specs=(
            P(("groups", "attn"), "expert"),
            P(("groups", "attn"), None),
            P(("groups", "attn"), None),
            P("attn", "expert", None),
            P("attn", "expert", None),
            P("attn", None, "expert"),
            P(("groups", "attn", "expert"), None, None),
            P(("groups", "attn", "expert"), None, None, None),
            P(("groups", "attn", "expert"), None, None, None),
            P(("groups", "attn", "expert")),
        ),
        out_specs=(P(("groups", "attn"), "expert"), P(("groups", "attn", "expert"), None)),
        check_vma=False,
    )
```

```python
import functools

import jax
import jax.numpy as jnp
from jax import lax
from jax.experimental import pallas as pl
from jax.experimental.pallas import tpu as pltpu
from jax.sharding import PartitionSpec as P

F32 = jnp.float32
BF16 = jnp.bfloat16
I32 = jnp.int32

TOKEN_CUTS = 4
CHUNK_ROWS = 16
LAG = 3
HLAG = 8
PACE = 2
RETURN_CUTS = 4
RETURN_DELAY = 1


def remote(src, dst, send_sem, recv_sem, axis, peer):
    return pltpu.make_async_remote_copy(
        src_ref=src,
        dst_ref=dst,
        send_sem=send_sem,
        recv_sem=recv_sem,
        device_id={axis: peer},
        device_id_type=pl.DeviceIdType.MESH,
    )


def attend(s, length, query_ref, ck_ref, cv_ref, att_ref, kv_count):
    _, heads, size = query_ref.shape
    span = ck_ref.shape[1]
    column = lax.broadcasted_iota(I32, (heads, span), 1)
    row = lax.broadcasted_iota(I32, (heads, span), 0)
    own = lax.rem(column, kv_count) == row // (heads // kv_count)
    scores = lax.dot_general(
        query_ref[s], ck_ref[s], (((1,), (1,)), ((), ())),
        preferred_element_type=F32,
    ) * size ** (-0.5)
    live = own & (column < length * kv_count)
    masked = jnp.where(live, scores, -jnp.inf)
    peak = jnp.max(masked, axis=1, keepdims=True)
    weighted = jnp.exp(masked - peak)
    prob = (weighted / jnp.sum(weighted, axis=1, keepdims=True)).astype(BF16)
    att_ref[s] = jnp.dot(prob, cv_ref[s], preferred_element_type=F32).astype(BF16)


def moe_kernel(
    n_attn,
    n_exp,
    experts,
    kv_count,
    tok_hbm,
    ids_hbm,
    gw_hbm,
    wg_hbm,
    wu_hbm,
    wd_hbm,
    length_hbm,
    query_hbm,
    ck_hbm,
    cv_hbm,
    out_hbm,
    att_hbm,
    out_ref,
    att_ref,
    wg,
    wu,
    wd,
    ck,
    cv,
    query,
    length,
    tok_all,
    ids_all,
    gw_all,
    pos,
    gate_of,
    part,
    part_in,
    hid,
    acc,
    packed,
    chosen,
    final,
    early,
    res,
    ret1,
    ret1_in,
    ret2,
    ret2_in,
    w_sem,
    c_sem,
    out_sem,
    ids_s,
    ids_r,
    gw_s,
    gw_r,
    far_s,
    far_r,
    near_s,
    near_r,
    part_s,
    part_r,
    hid_s,
    ret1_s,
    ret1_r,
    ret2_s,
    ret2_r,
):
    me = lax.axis_index("attn")
    mine = lax.axis_index("expert")
    lane = lax.rem(me, 2)
    line = me // 2
    lines = n_attn // 2
    partner = me + 1 - 2 * lane
    last = n_exp - 1
    local = wg.shape[0]
    rows, feat = tok_all.shape[1:]
    ffn = wg.shape[2]
    feat_out = wd.shape[2]
    topk = ids_all.shape[1]
    half = part.shape[2]
    capacity = 2 * half
    all_rows = n_attn * rows
    per = half // CHUNK_ROWS
    chunks = local * per
    cut = feat // TOKEN_CUTS
    out_cut = feat_out // RETURN_CUTS

    def at_line(other):
        return lax.rem(other + 2 * lines, lines)

    tok_copy = pltpu.make_async_copy(tok_hbm, tok_all.at[lines + line], c_sem.at[0])
    ids_copy = pltpu.make_async_copy(ids_hbm, ids_all.at[me], c_sem.at[1])
    gw_copy = pltpu.make_async_copy(gw_hbm, gw_all.at[me], c_sem.at[2])
    len_copy = pltpu.make_async_copy(length_hbm, length, c_sem.at[3])
    query_copy = pltpu.make_async_copy(query_hbm, query, c_sem.at[4])
    ck_copy = pltpu.make_async_copy(ck_hbm, ck, c_sem.at[5])
    cv_copy = pltpu.make_async_copy(cv_hbm, cv, c_sem.at[6])
    for copy in (ids_copy, gw_copy, tok_copy):
        copy.start()

    barrier = pltpu.get_barrier_semaphore()
    for d in range(1, n_attn):
        pl.semaphore_signal(
            barrier, inc=1, device_id={"attn": lax.rem(me + d, n_attn)},
            device_id_type=pl.DeviceIdType.MESH,
        )

    @pl.when(mine > 0)
    def _():
        pl.semaphore_signal(
            barrier, inc=1, device_id={"expert": mine - 1},
            device_id_type=pl.DeviceIdType.MESH,
        )

    @pl.when(mine < last)
    def _():
        pl.semaphore_signal(
            barrier, inc=1, device_id={"expert": mine + 1},
            device_id_type=pl.DeviceIdType.MESH,
        )

    ends = jnp.where(mine > 0, 1, 0) + jnp.where(mine < last, 1, 0)
    ids_copy.wait()
    gw_copy.wait()
    tok_copy.wait()
    for copy in (query_copy, len_copy, ck_copy, cv_copy):
        copy.start()

    def weight_copy(i, j):
        src, dst = ((wg_hbm, wg), (wu_hbm, wu), (wd_hbm, wd))[i]
        return pltpu.make_async_copy(src.at[j], dst.at[j], w_sem.at[i, j])

    for j in range(local):
        weight_copy(0, j).start()
        weight_copy(1, j).start()
    for j in range(local):
        weight_copy(2, j).start()

    pl.semaphore_wait(barrier, n_attn - 1 + ends)

    def ids_send(d, slot):
        return remote(ids_all.at[slot], ids_all.at[slot], ids_s.at[d - 1], ids_r.at[d - 1],
                      "attn", lax.rem(me + d, n_attn))

    def gw_send(d, slot):
        return remote(gw_all.at[slot], gw_all.at[slot], gw_s.at[d - 1], gw_r.at[d - 1],
                      "attn", lax.rem(me + d, n_attn))

    def far(d, q, block):
        view = tok_all.at[lines + block, :, pl.ds(q * cut, cut)]
        return remote(view, view, far_s.at[d - 1, q], far_r.at[d - 1, q],
                      "attn", at_line(line + d) * 2 + lane)

    def near(d, q):
        block = at_line(line - d)
        columns = pl.ds(q * cut, cut)
        return remote(tok_all.at[lines + block, :, columns], tok_all.at[block, :, columns],
                      near_s.at[d, q], near_r.at[d, q], "attn", partner)

    for d in range(1, n_attn):
        ids_send(d, me).start()
        gw_send(d, me).start()
    for q in range(TOKEN_CUTS):
        for d in range(1, lines):
            far(d, q, line).start()
    for q in range(TOKEN_CUTS):
        near(0, q).start()

    acc[...] = jnp.zeros_like(acc)

    for d in range(1, n_attn):
        ids_send(d, lax.rem(me + n_attn - d, n_attn)).wait_recv()
        gw_send(d, lax.rem(me + n_attn - d, n_attn)).wait_recv()

    before = (
        lax.broadcasted_iota(I32, (rows, rows), 0)
        < lax.broadcasted_iota(I32, (rows, rows), 1)
    ).astype(F32).astype(BF16)
    names = lax.broadcasted_iota(I32, (experts, rows), 0)
    offset = jnp.zeros((experts, 1), F32)
    for b in range(n_attn):
        member = jnp.zeros((experts, rows), F32)
        factor = jnp.zeros((experts, rows), F32)
        wide = gw_all[b].astype(F32)
        for k in range(topk):
            hit = names == ids_all[b, k:k + 1, :]
            member = jnp.where(hit, 1.0, member)
            factor = jnp.where(hit, wide[k:k + 1, :], factor)
        place = jnp.dot(member.astype(BF16), before, preferred_element_type=F32) + offset
        offset = offset + jnp.sum(member, axis=1, keepdims=True)
        here = lax.rem(b + lane + 1, 2) * lines + b // 2
        columns = pl.ds(pl.multiple_of(here * rows, rows), rows)
        pos[:, columns] = jnp.where(member > 0.5, place, -1.0).astype(I32)
        gate_of[:, columns] = factor

    def spread_of(j):
        place = pos[pl.ds(me * local + j, 1), :]
        factor = gate_of[pl.ds(me * local + j, 1), :]
        slots = lax.broadcasted_iota(I32, (capacity, all_rows), 0)
        return jnp.where(slots == place, factor, 0.0)

    def relay(q):
        for d in range(1, lines):
            far(d, q, at_line(line - d)).wait_recv()
            near(d, q).start()

    def chosen_of(j):
        place = pos[pl.ds(me * local + j, 1), :]
        slots = lax.broadcasted_iota(I32, (capacity, all_rows), 0)
        return (slots == place).astype(F32).astype(BF16)

    def start_first(q):
        for d in range(lines):
            near(d, q).wait_recv()
        columns = slice(q * cut, (q + 1) * cut)
        narrow = jnp.dot(
            chosen[...], tok_all[:, :, columns].reshape(all_rows, cut),
            preferred_element_type=F32,
        ).astype(BF16)
        for w, to in ((wg, 0), (wu, ffn)):
            term = jnp.dot(narrow, w[0, columns, :], preferred_element_type=F32)
            if q > 0:
                term = term + early[:, to:to + ffn]
            if q < TOKEN_CUTS - 1:
                early[:, to:to + ffn] = term
            else:
                part[0, :, :, to:to + ffn] = term.astype(BF16).reshape(2, half, ffn)

    chosen[...] = chosen_of(0)
    final[...] = spread_of(local - 1).T.astype(BF16)
    relay(0)
    weight_copy(0, 0).wait()
    weight_copy(1, 0).wait()
    for q in range(1, TOKEN_CUTS):
        relay(q)
        start_first(q - 1)
    start_first(TOKEN_CUTS - 1)

    def steps_from(way):
        return mine + way * (last - 2 * mine)

    near_way = 2 * mine // n_exp

    def piece(ref, way, k):
        j = k // per
        first_row = pl.multiple_of(lax.rem(k, per) * CHUNK_ROWS, CHUNK_ROWS)
        return ref.at[j, way, pl.ds(first_row, CHUNK_ROWS)]

    def part_copy(way, k):
        return remote(piece(part, way, k), piece(part_in, way, k),
                      part_s.at[way, k // per], part_r.at[way, k],
                      "expert", lax.rem(mine + 1 - 2 * way + n_exp, n_exp))

    def hid_copy(way, k):
        return remote(piece(hid, way, k), piece(hid, way, k),
                      hid_s.at[way, k // per], part_r.at[way, k],
                      "expert", lax.rem(mine - 1 + 2 * way + n_exp, n_exp))

    def send_parts(j):
        for way in range(2):
            @pl.when(steps_from(way) == 0)
            def _():
                for r in range(per):
                    part_copy(way, j * per + r).start()

    def pack(j):
        packed[...] = jnp.dot(
            chosen_of(j), tok_all[...].reshape(all_rows, feat),
            preferred_element_type=F32,
        ).astype(BF16)

    def project(j, i):
        weight_copy(i, j).wait()
        w = (wg, wu)[i]
        some = jnp.dot(packed[...], w[j], preferred_element_type=F32).astype(BF16)
        part[j, :, :, i * ffn:(i + 1) * ffn] = some.reshape(2, half, ffn)

    def first(j, carry):
        pack(j)
        project(j, 0)
        project(j, 1)
        send_parts(j)
        return carry

    send_parts(0)
    lax.fori_loop(1, local - 1, first, 0)

    def reduce(way, k):
        part_copy(way, k).wait_recv()
        total = piece(part, way, k)[...].astype(F32) + piece(part_in, way, k)[...].astype(F32)

        @pl.when(steps_from(way) < last)
        def _():
            piece(part, way, k)[...] = total.astype(BF16)
            part_copy(way, k).start()

        @pl.when(steps_from(way) == last)
        def _():
            gate = total[:, :ffn]
            piece(hid, way, k)[...] = (
                gate / (1.0 + jnp.exp(-gate)) * total[:, ffn:]
            ).astype(BF16)
            hid_copy(way, k).start()

    def reduce_step(s, carry):
        for way in (near_way, 1 - near_way):
            k = s - LAG * (steps_from(way) - 1)

            @pl.when((steps_from(way) > 0) & (k >= 0) & (k < chunks))
            def _():
                reduce(way, k)
        return carry

    def pass_on(s, carry):
        for way in (1 - near_way, near_way):
            hops = last - steps_from(way)
            k = s - HLAG * (hops - 1)
            due = (hops > 0) & (k >= 0) & (k < chunks)

            @pl.when(due)
            def _():
                hid_copy(way, k).wait_recv()

            @pl.when(due & (hops < last))
            def _():
                hid_copy(way, k).start()
        return carry

    ahead = HLAG * (last - 1)
    over = LAG * (last - 1)

    def both_steps(s, carry):
        reduce_step(s, carry)
        for i in range(PACE):
            pass_on((s - chunks) * PACE + i, carry)
        return carry

    reduce_step(0, 0)
    pack(local - 1)
    reduce_step(1, 0)
    project(local - 1, 0)
    reduce_step(2, 0)
    project(local - 1, 1)
    send_parts(local - 1)
    lax.fori_loop(3, chunks, reduce_step, 0)
    lax.fori_loop(chunks, chunks + over, both_steps, 0)
    lax.fori_loop(min(over * PACE, ahead), ahead, pass_on, 0)

    def combine(spread, result):
        return lax.dot_general(
            spread, result, (((0,), (0,)), ((), ())), preferred_element_type=F32
        )

    def second(j, carry):
        lax.fori_loop(jnp.maximum(ahead + j * per, over * PACE), ahead + (j + 1) * per, pass_on, 0)
        weight_copy(2, j).wait()
        result = jnp.dot(
            hid[j].reshape(capacity, ffn), wd[j], preferred_element_type=F32
        ).astype(BF16)
        acc[...] += combine(spread_of(j).astype(BF16), result)
        return carry

    lax.fori_loop(0, local - 1, second, 0)
    j = local - 1
    weight_copy(2, j).wait()
    lax.fori_loop(ahead + j * per, ahead + (j + 1) * per, pass_on, 0)

    split = all_rows // 2

    def ret1_copy(q):
        columns = pl.ds(q * out_cut, out_cut)
        return remote(ret1.at[:, columns], ret1_in.at[:, columns],
                      ret1_s.at[q], ret1_r.at[q], "attn", partner)

    def ret2_copy(d, q):
        columns = pl.ds(q * out_cut, out_cut)
        return remote(ret2.at[d - 1, :, columns], ret2_in.at[d - 1, :, columns],
                      ret2_s.at[d - 1, q], ret2_r.at[d - 1, q],
                      "attn", at_line(line + d) * 2 + lane)

    def columns_of(q):
        return slice(q * out_cut, (q + 1) * out_cut)

    def own(index, q):
        return pl.ds(pl.multiple_of(split + index * rows, rows), rows), columns_of(q)

    def got(index, q):
        return pl.ds(pl.multiple_of(index * rows, rows), rows), columns_of(q)

    def to_partner(q):
        columns = columns_of(q)
        result = jnp.dot(
            hid[j].reshape(capacity, ffn), wd[j, :, columns], preferred_element_type=F32
        ).astype(BF16)
        res[:, columns] = result
        ret1[:, columns] = (acc[:split, columns] + jnp.dot(final[:split], result, preferred_element_type=F32)).astype(BF16)
        ret1_copy(q).start()

    def to_lines(q):
        columns = columns_of(q)
        acc[split:, columns] += jnp.dot(
            final[split:], res[:, columns], preferred_element_type=F32
        )
        ret1_copy(q).wait_recv()
        for d in range(1, lines):
            to = at_line(line + d)
            ret2[d - 1, :, columns] = (
                acc[own(to, q)] + ret1_in[got(to, q)].astype(F32)
            ).astype(BF16)
            ret2_copy(d, q).start()

    for q in range(RETURN_CUTS):
        to_partner(q)
        if q >= RETURN_DELAY:
            to_lines(q - RETURN_DELAY)
    for q in range(max(RETURN_CUTS - RETURN_DELAY, 0), RETURN_CUTS):
        to_lines(q)
    att_copy = pltpu.make_async_copy(att_ref, att_hbm, c_sem.at[7])
    for copy in (len_copy, query_copy, ck_copy, cv_copy):
        copy.wait()
    for s in range(query.shape[0]):
        attend(s, length[s], query, ck, cv, att_ref, kv_count)
    att_copy.start()

    def out_copy(q):
        columns = pl.ds(q * out_cut, out_cut)
        return pltpu.make_async_copy(out_ref.at[:, columns], out_hbm.at[:, columns], out_sem.at[q])

    for q in range(RETURN_CUTS):
        total = acc[own(line, q)] + ret1_in[got(line, q)].astype(F32)
        for d in range(1, lines):
            ret2_copy(d, q).wait_recv()
            total = total + ret2_in[d - 1, :, columns_of(q)].astype(F32)
        out_ref[:, columns_of(q)] = total.astype(BF16)
        out_copy(q).start()

    for d in range(1, n_attn):
        ids_send(d, me).wait_send()
        gw_send(d, me).wait_send()
    for q in range(TOKEN_CUTS):
        near(0, q).wait_send()
        for d in range(1, lines):
            far(d, q, line).wait_send()
            near(d, q).wait_send()
    for q in range(RETURN_CUTS):
        ret1_copy(q).wait_send()
        for d in range(1, lines):
            ret2_copy(d, q).wait_send()

    att_copy.wait()
    for q in range(RETURN_CUTS):
        out_copy(q).wait()

    for way in range(2):
        for j in range(local):
            @pl.when(steps_from(way) < last)
            def _():
                remote(part.at[j, way], part_in.at[j, way], part_s.at[way, j], part_r.at[way, 0],
                       "expert", lax.rem(mine + 1 - 2 * way + n_exp, n_exp)).wait_send()

            @pl.when(steps_from(way) > 0)
            def _():
                remote(hid.at[j, way], hid.at[j, way], hid_s.at[way, j], part_r.at[way, 0],
                       "expert", lax.rem(mine - 1 + 2 * way + n_exp, n_exp)).wait_send()


def routed(tokens, expert_ids, gate_weight, w_gate, w_up, w_down, query, cache_k, cache_v, lengths, n_attn, n_exp):
    rows, feat = tokens.shape
    local, _, ffn = w_gate.shape
    feat_out = w_down.shape[2]
    topk = expert_ids.shape[1]
    experts = local * n_attn
    capacity = rows * topk // local
    half = capacity // 2
    lines = n_attn // 2
    chunks = local * (half // CHUNK_ROWS)
    seqs, heads, size = query.shape
    context, kv_count = cache_k.shape[1:3]
    flat = (seqs, context * kv_count, size)
    dma = pltpu.SemaphoreType.DMA
    vmem = pltpu.VMEM
    return pl.pallas_call(
        functools.partial(moe_kernel, n_attn, n_exp, experts, kv_count),
        out_shape=(
            jax.ShapeDtypeStruct((rows, feat_out), BF16),
            jax.ShapeDtypeStruct(query.shape, BF16),
        ),
        in_specs=[pl.BlockSpec(memory_space=pltpu.HBM)] * 10,
        out_specs=[pl.BlockSpec(memory_space=pltpu.HBM)] * 2,
        scratch_shapes=[
            vmem((rows, feat_out), BF16),
            vmem(query.shape, BF16),
            vmem(w_gate.shape, BF16),
            vmem(w_up.shape, BF16),
            vmem(w_down.shape, BF16),
            vmem(flat, BF16),
            vmem(flat, BF16),
            vmem(query.shape, BF16),
            pltpu.SMEM(lengths.shape, I32),
            vmem((n_attn, rows, feat), BF16),
            vmem((n_attn, topk, rows), I32),
            vmem((n_attn, topk, rows), BF16),
            vmem((experts, n_attn * rows), I32),
            vmem((experts, n_attn * rows), F32),
            vmem((local, 2, half, 2 * ffn), BF16),
            vmem((local, 2, half, 2 * ffn), BF16),
            vmem((local, 2, half, ffn), BF16),
            vmem((n_attn * rows, feat_out), F32),
            vmem((capacity, feat), BF16),
            vmem((capacity, n_attn * rows), BF16),
            vmem((n_attn * rows, capacity), BF16),
            vmem((capacity, 2 * ffn), F32),
            vmem((capacity, feat_out), BF16),
            vmem((lines * rows, feat_out), BF16),
            vmem((lines * rows, feat_out), BF16),
            vmem((lines - 1, rows, feat_out), BF16),
            vmem((lines - 1, rows, feat_out), BF16),
            dma((3, local)),
            dma((8,)),
            dma((RETURN_CUTS,)),
            dma((n_attn - 1,)),
            dma((n_attn - 1,)),
            dma((n_attn - 1,)),
            dma((n_attn - 1,)),
            dma((lines - 1, TOKEN_CUTS)),
            dma((lines - 1, TOKEN_CUTS)),
            dma((lines, TOKEN_CUTS)),
            dma((lines, TOKEN_CUTS)),
            dma((2, local)),
            dma((2, chunks)),
            dma((2, local)),
            dma((RETURN_CUTS,)),
            dma((RETURN_CUTS,)),
            dma((lines - 1, RETURN_CUTS)),
            dma((lines - 1, RETURN_CUTS)),
        ],
        compiler_params=pltpu.CompilerParams(
            collective_id=0, has_side_effects=True, vmem_limit_bytes=56 * 1024 * 1024
        ),
    )(
        tokens, expert_ids.T, gate_weight.T, w_gate, w_up, w_down, lengths, query,
        cache_k.reshape(flat), cache_v.reshape(flat),
    )


def finish_kernel(moe_ref, att_ref, out_ref, attn_out_ref):
    heads, size = att_ref.shape[1:]
    out_ref[...] = moe_ref[...]
    for h in range(heads):
        attn_out_ref[:, h * size:(h + 1) * size] = att_ref[:, h, :]


def finish(moe, att):
    seqs, heads, size = att.shape
    return pl.pallas_call(
        finish_kernel,
        out_shape=(
            jax.ShapeDtypeStruct(moe.shape, moe.dtype),
            jax.ShapeDtypeStruct((seqs, heads * size), att.dtype),
        ),
        in_specs=[pl.BlockSpec(memory_space=pltpu.VMEM)] * 2,
        out_specs=[pl.BlockSpec(memory_space=pltpu.VMEM)] * 2,
    )(moe, att)


def body(tokens, expert_ids, gate_weight, w_gate, w_up, w_down, query, cache_k, cache_v, lengths):
    n_attn = lax.axis_size("attn")
    n_exp = lax.axis_size("expert")
    moe_out, attended = routed(
        tokens, expert_ids, gate_weight, w_gate, w_up, w_down,
        query, cache_k, cache_v, lengths, n_attn, n_exp,
    )
    return finish(moe_out, attended)


def solution(mesh):
    return jax.shard_map(
        body,
        mesh=mesh,
        in_specs=(
            P(("groups", "attn"), "expert"),
            P(("groups", "attn"), None),
            P(("groups", "attn"), None),
            P("attn", "expert", None),
            P("attn", "expert", None),
            P("attn", None, "expert"),
            P(("groups", "attn", "expert"), None, None),
            P(("groups", "attn", "expert"), None, None, None),
            P(("groups", "attn", "expert"), None, None, None),
            P(("groups", "attn", "expert")),
        ),
        out_specs=(P(("groups", "attn"), "expert"), P(("groups", "attn", "expert"), None)),
        check_vma=False,
    )
```
